128 devices in a mesh: tp: 16 (over z, y), dp: 8 (over x, core).
Axes of the slice: x: 4, y: 4, z: 4, core: 2. Of those that a mesh axis runs over, the one named last changes fastest.
Arguments:
- hidden: bfloat16 [2048, 2048], P('dp')
- embedding: bfloat16 [128256, 2048], P('tp')
- norm_weight: float32 [2048], replicated
- teach_ids: int32 [2048, 256], P('dp')
- teach_prob: float32 [2048, 256], P('dp')
- tok_mask: float32 [2048], P('dp')
Outputs:
- output 1: float32 [], replicated
- output 2: bfloat16 [2048, 2048], P('dp')
- output 3: float32 [128256, 2048], P('tp', 'dp')
- output 4: float32 [2048], replicated
All inputs are finite; a program needn't handle non-finite values.
Results may differ from the reference program's by a relative error of at most 0.001.
Values sent between devices are 32-bit elements.
A program may use at most 1 GiB of HBM per device.

```python
import jax
import jax.numpy as jnp
from jax import lax

MODEL_DIM = 2048
VOCAB_SIZE = 128256
TEACH_TOP = 256
NUM_TOKENS = 2048

EPS_NORM = 1e-6
LOGIT_GAIN = 2.5
HALF_TOP = TEACH_TOP // 2
FREQ_VOCAB = VOCAB_SIZE // 8
ROW_BLOCK = min(NUM_TOKENS, 64)


def draw_teacher_ids(key_ids):
    key_low, key_high, key_perm = jax.random.split(key_ids, 3)
    low_band = FREQ_VOCAB // HALF_TOP
    high_band = (VOCAB_SIZE - FREQ_VOCAB) // HALF_TOP
    slot_pos = jnp.arange(HALF_TOP, dtype=jnp.int32)
    high_width = jnp.where(slot_pos == HALF_TOP - 1, VOCAB_SIZE - FREQ_VOCAB - (HALF_TOP - 1) * high_band, high_band)
    low_off = jax.random.randint(key_low, (NUM_TOKENS, HALF_TOP), 0, low_band, dtype=jnp.int32)
    high_raw = jax.random.randint(key_high, (NUM_TOKENS, HALF_TOP), 0, 1 << 24, dtype=jnp.int32)
    high_off = high_raw % high_width[None, :]
    low_off = low_off.at[0, 0].set(0)
    high_off = high_off.at[0, HALF_TOP - 1].set(high_width[HALF_TOP - 1] - 1)
    low_ids = slot_pos[None, :] * low_band + low_off
    high_ids = FREQ_VOCAB + slot_pos[None, :] * high_band + high_off
    all_ids = jnp.concatenate([low_ids, high_ids], axis=1)
    row_keys = jax.random.split(key_perm, NUM_TOKENS)
    perm_rows = jax.vmap(lambda row_key: jax.random.permutation(row_key, TEACH_TOP))(row_keys)
    return jnp.take_along_axis(all_ids, perm_rows.astype(jnp.int32), axis=1)


def draw_mask(key_mask):
    keep_flag = jax.random.randint(key_mask, (NUM_TOKENS,), 0, 8, dtype=jnp.int32) != 0
    return keep_flag.astype(jnp.float32).at[0].set(1.0)


def setup_inputs(seed: int = 0) -> dict:
    root_key = jax.random.key(seed)
    key_h, key_e, key_w, key_ids, key_prob, key_mask = jax.random.split(root_key, 6)
    hidden = jax.random.normal(key_h, (NUM_TOKENS, MODEL_DIM), jnp.float32).astype(jnp.bfloat16)
    embed_scale = LOGIT_GAIN * MODEL_DIM ** -0.5
    embedding = (jax.random.normal(key_e, (VOCAB_SIZE, MODEL_DIM), jnp.float32) * embed_scale).astype(jnp.bfloat16)
    norm_weight = 0.5 * jax.random.normal(key_w, (MODEL_DIM,), jnp.float32)
    teach_ids = draw_teacher_ids(key_ids)
    teach_prob = jax.nn.softmax(jax.random.normal(key_prob, (NUM_TOKENS, TEACH_TOP), jnp.float32), axis=1)
    tok_mask = draw_mask(key_mask)
    return {'hidden': hidden, 'embedding': embedding, 'norm_weight': norm_weight, 'teach_ids': teach_ids, 'teach_prob': teach_prob, 'tok_mask': tok_mask}


def reference(hidden, embedding, norm_weight, teach_ids, teach_prob, tok_mask):
    mask_total = jnp.sum(tok_mask)
    scale_w = 1.0 + norm_weight
    num_blocks = NUM_TOKENS // ROW_BLOCK
    row_ids = jnp.arange(ROW_BLOCK)[:, None]

    def block_step(acc_embed, block_in):
        h_blk, ids_blk, prob_blk, mask_blk = block_in
        h_f32 = h_blk.astype(jnp.float32)
        inv_rms = lax.rsqrt(jnp.mean(h_f32 * h_f32, axis=1, keepdims=True) + EPS_NORM)
        normed = h_f32 * inv_rms
        normed_bf = (normed * scale_w).astype(jnp.bfloat16)
        logits = lax.dot_general(normed_bf, embedding, (((1,), (1,)), ((), ())), preferred_element_type=jnp.float32)
        row_max = jnp.max(logits, axis=1, keepdims=True)
        log_norm = row_max + jnp.log(jnp.sum(jnp.exp(logits - row_max), axis=1, keepdims=True))
        picked = jnp.take_along_axis(logits, ids_blk, axis=1)
        teach_sum = jnp.sum(prob_blk * picked, axis=1)
        loss_part = jnp.sum(mask_blk * (teach_sum - log_norm[:, 0]))
        weight = (mask_blk / mask_total)[:, None]
        soft_prob = jnp.exp(logits - log_norm)
        d_logits = (soft_prob * weight).at[row_ids, ids_blk].add(-prob_blk * weight)
        dlogit_bf = d_logits.astype(jnp.bfloat16)
        grad_u = jnp.dot(dlogit_bf, embedding, preferred_element_type=jnp.float32)
        acc_embed = acc_embed + lax.dot_general(dlogit_bf, normed_bf, (((0,), (0,)), ((), ())), preferred_element_type=jnp.float32)
        d_normed = grad_u * scale_w
        grad_h = inv_rms * (d_normed - normed * jnp.mean(d_normed * normed, axis=1, keepdims=True))
        grad_w = jnp.sum(grad_u * normed, axis=0)
        return acc_embed, (loss_part, grad_h.astype(jnp.bfloat16), grad_w)

    blocks = (hidden.reshape(num_blocks, ROW_BLOCK, MODEL_DIM), teach_ids.reshape(num_blocks, ROW_BLOCK, TEACH_TOP), teach_prob.reshape(num_blocks, ROW_BLOCK, TEACH_TOP), tok_mask.reshape(num_blocks, ROW_BLOCK))
    acc_init = jnp.zeros((VOCAB_SIZE, MODEL_DIM), jnp.float32)
    grad_embed, (loss_parts, grad_hidden, norm_parts) = lax.scan(block_step, acc_init, blocks)
    loss_mean = -jnp.sum(loss_parts) / mask_total
    return loss_mean, grad_hidden.reshape(NUM_TOKENS, MODEL_DIM), grad_embed, jnp.sum(norm_parts, axis=0)
```

```python
import functools

import jax
import jax.numpy as jnp
import numpy as np
from jax import lax
from jax.experimental import pallas as pl
from jax.experimental.pallas import tpu as pltpu
from jax.sharding import Mesh
from jax.sharding import PartitionSpec as P


EPS_NORM = 1e-6
NEG = -1e30
BIG = 1e30
F32 = jnp.float32
BF16 = jnp.bfloat16
I32 = jnp.int32
SLOTS = 8
FAST = 2
VB = 256
VB1 = 512
VMEM_LIMIT = 60 * 1024 * 1024
MESH = pl.DeviceIdType.MESH


def params(**kw):
    return pltpu.CompilerParams(vmem_limit_bytes=VMEM_LIMIT, **kw)


def cost(flops, nbytes, trans=0):
    return pl.CostEstimate(flops=int(flops), bytes_accessed=int(nbytes), transcendentals=int(trans))


def sort_kernel(ids_ref, pt_ref, mask_ref, out_ref):
    n = ids_ref.shape[1]
    sub = lax.broadcasted_iota(I32, (8, 128), 0)
    for g in range(ids_ref.shape[0] // 128):
        cols = slice(g * 128, (g + 1) * 128)
        key = (ids_ref[cols, :] + 1).astype(F32).T
        prob = pt_ref[cols, :].T
        k = [key[8 * a:8 * a + 8, :] for a in range(n // 8)]
        p = [prob[8 * a:8 * a + 8, :] for a in range(n // 8)]
        size = 2
        while size <= n:
            j = size // 2
            while j >= 1:
                if j >= 8:
                    for a in range(n // 8):
                        if (8 * a) & j:
                            continue
                        b = a + j // 8
                        up = ((8 * a) & size) == 0
                        swap = k[a] > k[b] if up else k[a] < k[b]
                        lo, hi = jnp.minimum(k[a], k[b]), jnp.maximum(k[a], k[b])
                        k[a], k[b] = (lo, hi) if up else (hi, lo)
                        p[a], p[b] = jnp.where(swap, p[b], p[a]), jnp.where(swap, p[a], p[b])
                else:
                    low = (sub & j) == 0
                    for a in range(n // 8):
                        if size >= 8:
                            up = ((8 * a) & size) == 0
                            want_min = low if up else (sub & j) != 0
                        else:
                            want_min = ((sub & j) == 0) == ((sub & size) == 0)
                        ka = jnp.where(low, pltpu.roll(k[a], 8 - j, 0), pltpu.roll(k[a], j, 0))
                        pa = jnp.where(low, pltpu.roll(p[a], 8 - j, 0), pltpu.roll(p[a], j, 0))
                        new = jnp.where(want_min, jnp.minimum(k[a], ka), jnp.maximum(k[a], ka))
                        p[a] = jnp.where(new == ka, pa, p[a])
                        k[a] = new
                j //= 2
            size *= 2
        sign = jnp.where(mask_ref[:, cols] > 0, 1.0, -1.0)
        for a in range(n // 8):
            out_ref[8 * a:8 * a + 8, cols] = k[a] * sign
            out_ref[n + 8 * a:n + 8 * a + 8, cols] = p[a]


def sort_lists(ids, prob, mask):
    tokens, top = ids.shape
    return pl.pallas_call(
        sort_kernel,
        out_shape=jax.ShapeDtypeStruct((2 * top, tokens), F32),
        in_specs=[pl.BlockSpec(memory_space=pltpu.VMEM)] * 3,
        out_specs=pl.BlockSpec(memory_space=pltpu.VMEM),
        compiler_params=params(),
        cost_estimate=cost(4e9, 4 * 4 * tokens * top),
        name='sort_lists',
    )(ids, prob, mask[None, :])


def expand_kernel(nblk, sc_ref, list_ref, w_ref, tabr_ref, tabp_ref, cnt_ref, loc_ref, pw_ref):
    base, rows = sc_ref[0], sc_ref[1]
    top = list_ref.shape[0] // 2
    nq = top // 8
    sub = lax.broadcasted_iota(I32, (8, 128), 0)
    w = w_ref[...]
    over = jnp.zeros((8, 128), I32)
    prev = None
    for q in range(nq):
        ids = jnp.abs(list_ref[8 * q:8 * q + 8, :]).astype(I32) - 1 - base
        ok = (ids >= 0) & (ids < rows)
        loc = jnp.where(ok, ids, -1)
        loc_ref[8 * q:8 * q + 8, :] = loc
        pw_ref[8 * q:8 * q + 8, :] = list_ref[top + 8 * q:top + 8 * q + 8, :] * w
        blk = loc >> 7
        if prev is not None:
            over = jnp.where((blk == prev) & ok, 1, over)
        prev = blk
    for sh in (4, 2, 1):
        over = jnp.maximum(over, pltpu.roll(over, sh, 0))
    tile = min(nblk, 8)

    def body(bt, carry):
        b0 = bt * tile
        accc = [jnp.full((8, 128), -1, I32)] * tile
        accp = [jnp.zeros((8, 128), F32)] * tile
        for q in range(nq):
            loc = loc_ref[8 * q:8 * q + 8, :]
            blk = (loc >> 7) - b0
            code = (sub + 8 * q) * 128 + (loc & 127)
            p = pw_ref[8 * q:8 * q + 8, :]
            for i in range(tile):
                m = blk == i
                accc[i] = jnp.where(m, code, accc[i])
                accp[i] = jnp.where(m, p, accp[i])
        for i in range(tile):
            code, p = accc[i], accp[i]
            first = jnp.where(code >= 0, code, 1 << 24)
            for sh in (4, 2, 1):
                first = jnp.minimum(first, pltpu.roll(first, sh, 0))
            start = (first >> 7) & 7
            for sh in (1, 2, 4):
                move = (start & sh) != 0
                code = jnp.where(move, pltpu.roll(code, 8 - sh, 0), code)
                p = jnp.where(move, pltpu.roll(p, 8 - sh, 0), p)
            used = jnp.where(code >= 0, sub + 1, 0)
            for sh in (4, 2, 1):
                used = jnp.maximum(used, pltpu.roll(used, sh, 0))
            used = jnp.where(over > 0, SLOTS + 1, used)
            row = pl.multiple_of((b0 + i) * 8, 8)
            tabr_ref[pl.ds(row, 8), :] = jnp.where(code >= 0, code & 127, -1)
            tabp_ref[pl.ds(row, 8), :] = p
            cnt_ref[pl.ds(row, 8), :] = used
        return carry

    lax.fori_loop(0, nblk // tile, body, 0)


def expand(scal, lists, weight, nblk, list_map, groups):
    top = 256
    width = groups * 128
    full = jax.ShapeDtypeStruct((nblk * 8, width), F32)
    fulli = jax.ShapeDtypeStruct((nblk * 8, width), I32)
    tab = pl.BlockSpec((nblk * 8, 128), lambda g, s: (0, g))
    raw = pl.BlockSpec((top, 128), lambda g, s: (0, g))
    return pl.pallas_call(
        functools.partial(expand_kernel, nblk),
        out_shape=(fulli, full, fulli, jax.ShapeDtypeStruct((top, width), I32), jax.ShapeDtypeStruct((top, width), F32)),
        grid_spec=pltpu.PrefetchScalarGridSpec(
            num_scalar_prefetch=1,
            grid=(groups,),
            in_specs=[pl.BlockSpec((2 * top, 128), list_map), pl.BlockSpec((1, 128), lambda g, s: (0, g))],
            out_specs=(tab, tab, tab, raw, raw),
        ),
        compiler_params=params(),
        cost_estimate=cost(groups * 0.4e9, 4 * width * (4 * top + 3 * nblk * 8)),
    )(scal, lists, weight)


def fwd_kernel(own, sc_ref, *refs):
    ny = 2 if own else len(refs) - 6
    y_refs, (scale_ref, e_ref, z_ref, m_ref, s_ref, ut_ref) = refs[:ny], refs[ny:]
    i = pl.program_id(0)
    core, rows = sc_ref[3], sc_ref[1]
    step = 256

    @pl.when(i == 0)
    def _():
        scale = scale_ref[...]
        for a, y_ref in enumerate(y_refs):
            for r in range(0, y_ref.shape[0], step):
                u = (y_ref[r:r + step, :] * scale).astype(BF16).T
                if own:
                    slot = core if a == 0 else 1 - core
                    ut_ref[:, pl.ds(pl.multiple_of(slot * step, step), step)] = u
                else:
                    c0 = a * y_ref.shape[0] + r
                    ut_ref[:, c0:c0 + step] = u
        m_ref[...] = jnp.full(m_ref.shape, NEG, F32)
        s_ref[...] = jnp.zeros(s_ref.shape, F32)

    vb = e_ref.shape[0]
    left = rows - i * vb
    e = e_ref[...]
    nt = 512
    keep = lax.broadcasted_iota(I32, (vb, nt), 0) < left
    for c0 in range(0, ut_ref.shape[1], nt):
        cs = slice(c0, c0 + nt)
        z = jnp.dot(e, ut_ref[:, cs], preferred_element_type=F32)
        z = jnp.where(keep, z, NEG)
        z_ref[:, cs] = z
        z3 = z.reshape(vb // 8, 8, nt)
        old = m_ref[:, cs]
        new = jnp.maximum(old, jnp.max(z3, axis=0))
        m_ref[:, cs] = new
        s_ref[:, cs] = s_ref[:, cs] * jnp.exp(old - new) + jnp.sum(jnp.exp(z3 - new[None]), axis=0)


def forward(scal, ys, y_specs, scale, emb, half, width, own):
    dim = emb.shape[1]
    nb = half // VB
    stat = jax.ShapeDtypeStruct((8, width), F32)
    return pl.pallas_call(
        functools.partial(fwd_kernel, own),
        out_shape=(jax.ShapeDtypeStruct((half, width), F32), stat, stat),
        grid_spec=pltpu.PrefetchScalarGridSpec(
            num_scalar_prefetch=1,
            grid=(nb,),
            in_specs=list(y_specs) + [
                pl.BlockSpec((1, dim), lambda i, s: (0, 0)),
                pl.BlockSpec((VB, dim), lambda i, s: (s[3] * nb + i, 0)),
            ],
            out_specs=(
                pl.BlockSpec((VB, width), lambda i, s: (i, 0)),
                pl.BlockSpec((8, width), lambda i, s: (0, 0)),
                pl.BlockSpec((8, width), lambda i, s: (0, 0)),
            ),
            scratch_shapes=[pltpu.VMEM((dim, width), BF16)],
        ),
        compiler_params=params(dimension_semantics=('arbitrary',)),
        cost_estimate=cost(2.0 * half * width * dim, half * dim * 2 + half * width * 4 + width * dim * 4, half * width),
    )(scal, *ys, scale, emb)


def stats_kernel(tps, xs, groups, m_ref, s_ref, add_ref, lse_ref, tot_ref, send, recv, xrecv, ssem, rsem, xssem, xrsem):
    t, x, c = lax.axis_index('tp'), lax.axis_index('x'), lax.axis_index('core')
    me = t * 2 + c
    peers = tps * 2
    m = jnp.max(m_ref[...], axis=0, keepdims=True)
    s = jnp.sum(s_ref[...] * jnp.exp(m_ref[...] - m), axis=0, keepdims=True)
    send[...] = jnp.zeros(send.shape, F32)
    for g in range(groups):
        send[g:g + 1, :] = m[:, g * 128:(g + 1) * 128]
        send[groups + g:groups + g + 1, :] = s[:, g * 128:(g + 1) * 128]
    send[2 * groups:2 * groups + 1, :] = add_ref[...]

    barrier = pltpu.get_barrier_semaphore()

    def peer(j):
        r = lax.rem(me + j, peers)
        return {'tp': r // 2, 'core': lax.rem(r, 2)}

    def hello(j, carry):
        pl.semaphore_signal(barrier, inc=1, device_id=peer(j), device_id_type=MESH)
        return carry

    lax.fori_loop(1, peers, hello, 0)
    for j in range(1, xs):
        pl.semaphore_signal(barrier, inc=1, device_id={'x': lax.rem(x + j, xs)}, device_id_type=MESH)
    pl.semaphore_wait(barrier, peers - 1 + xs - 1)

    def copy(j):
        return pltpu.make_async_remote_copy(
            src_ref=send, dst_ref=recv.at[j], send_sem=ssem.at[j], recv_sem=rsem.at[j],
            device_id=peer(j), device_id_type=MESH)

    def xcopy(j):
        return pltpu.make_async_remote_copy(
            src_ref=send, dst_ref=xrecv.at[j], send_sem=xssem.at[j], recv_sem=xrsem.at[j],
            device_id={'x': lax.rem(x + j, xs)}, device_id_type=MESH)

    def start(j, carry):
        copy(j).start()
        return carry

    lax.fori_loop(1, peers, start, 0)
    for j in range(1, xs):
        xcopy(j).start()

    def finish(j, carry):
        copy(j).wait()
        return carry

    lax.fori_loop(1, peers, finish, 0)
    tot = send[2 * groups:2 * groups + 1, :]
    for j in range(1, xs):
        xcopy(j).wait()
        tot = tot + xrecv[j, 2 * groups:2 * groups + 1, :]
    tot_ref[...] = tot

    def most(j, best):
        return jnp.maximum(best, recv[j, 0:groups, :])

    best = lax.fori_loop(1, peers, most, send[0:groups, :])

    def add(j, acc):
        return acc + recv[j, groups:2 * groups, :] * jnp.exp(recv[j, 0:groups, :] - best)

    acc = lax.fori_loop(1, peers, add, send[groups:2 * groups, :] * jnp.exp(send[0:groups, :] - best))
    lse_ref[...] = best + jnp.log(acc)


def stats(m8, s8, add, tps, xs, cid):
    width = m8.shape[1]
    groups = width // 128
    rows = -(-(2 * groups + 1) // 8) * 8
    vm = pl.BlockSpec(memory_space=pltpu.VMEM)
    return pl.pallas_call(
        functools.partial(stats_kernel, tps, xs, groups),
        out_shape=(jax.ShapeDtypeStruct((groups, 128), F32), jax.ShapeDtypeStruct((1, 128), F32)),
        in_specs=[vm] * 3,
        out_specs=(vm, vm),
        scratch_shapes=[
            pltpu.VMEM((rows, 128), F32),
            pltpu.VMEM((2 * tps, rows, 128), F32),
            pltpu.VMEM((xs, rows, 128), F32),
            pltpu.SemaphoreType.DMA((2 * tps,)),
            pltpu.SemaphoreType.DMA((2 * tps,)),
            pltpu.SemaphoreType.DMA((xs,)),
            pltpu.SemaphoreType.DMA((xs,)),
        ],
        compiler_params=params(collective_id=cid, has_side_effects=True),
        cost_estimate=cost(2e9, 1 << 16),
    )(m8, s8, add)


def fill_teacher(cnt_ref, first, nrb, tabr_ref, tabp_ref, loc_hbm, pw_hbm, tm, loc_s, pw_s, sem):
    width = tm.shape[1]
    iota = lax.broadcasted_iota(I32, (128, 128), 0)
    for rb in range(nrb):
        n = cnt_ref[first + rb]

        def tile(g, carry):
            lanes = pl.ds(pl.multiple_of(g * 128, 128), 128)

            @pl.when(n <= SLOTS)
            def _():
                row = tabr_ref[8 * rb:8 * rb + 8, lanes]
                val = tabp_ref[8 * rb:8 * rb + 8, lanes]
                t = jnp.zeros((128, 128), F32)
                for s in range(SLOTS):
                    t = jnp.where(iota == row[s:s + 1, :], val[s:s + 1, :], t)
                tm[rb * 128:(rb + 1) * 128, lanes] = t

            @pl.when(n > SLOTS)
            def _():
                a = pltpu.make_async_copy(loc_hbm.at[:, lanes], loc_s, sem.at[0])
                b = pltpu.make_async_copy(pw_hbm.at[:, lanes], pw_s, sem.at[1])
                a.start()
                b.start()
                a.wait()
                b.wait()
                base = (first + rb) * 128

                def entries(k, t):
                    here = pl.ds(pl.multiple_of(k * 8, 8), 8)
                    row = loc_s[here, :] - base
                    val = pw_s[here, :]
                    for s in range(8):
                        t = jnp.where(iota == row[s:s + 1, :], val[s:s + 1, :], t)
                    return t

                tm[rb * 128:(rb + 1) * 128, lanes] = lax.fori_loop(
                    0, loc_s.shape[0] // 8, entries, jnp.zeros((128, 128), F32))

            return carry

        lax.fori_loop(0, width // 128, tile, 0)


def teacher_fast(tabr_ref, tabp_ref, rb, cs, n):
    iota = lax.broadcasted_iota(I32, (128, n), 0)
    t = jnp.zeros((128, n), F32)
    for s in range(FAST):
        row = tabr_ref[8 * rb + s:8 * rb + s + 1, cs]
        t = jnp.where(iota == row, tabp_ref[8 * rb + s:8 * rb + s + 1, cs], t)
    return t


def most_slots(cnt_ref, first, nrb):
    n = cnt_ref[first]
    for rb in range(1, nrb):
        n = jnp.maximum(n, cnt_ref[first + rb])
    return n


def du_kernel(sc_ref, cnt_ref, z_ref, c_ref, e_ref, tabr_ref, tabp_ref, loc_hbm, pw_hbm, du_ref, g_ref, tz_ref,
              tm, loc_s, pw_s, sem):
    i = pl.program_id(0)
    rows = sc_ref[1]
    vb, width = z_ref.shape
    nrb = vb // 128
    left = rows - i * vb

    @pl.when(i == 0)
    def _():
        du_ref[...] = jnp.zeros(du_ref.shape, F32)
        tz_ref[...] = jnp.zeros(tz_ref.shape, F32)

    slots = most_slots(cnt_ref, i * nrb, nrb)

    def make(teacher):
        for cs0 in range(0, width, 256):
            cs = slice(cs0, cs0 + 256)
            tz = jnp.zeros((8, 256), F32)
            for rb in range(nrb):
                rs = slice(rb * 128, (rb + 1) * 128)
                z = z_ref[rs, cs]
                t = teacher(rb, rs, cs)
                g_ref[rs, cs] = (jnp.exp(z - c_ref[:, cs]) - t).astype(BF16)
                tz = tz + jnp.sum((t * z).reshape(16, 8, 256), axis=0)
            tz_ref[:, cs] += tz

    @pl.when(slots <= FAST)
    def _():
        make(lambda rb, rs, cs: teacher_fast(tabr_ref, tabp_ref, rb, cs, 256))

    @pl.when(slots > FAST)
    def _():
        fill_teacher(cnt_ref, i * nrb, nrb, tabr_ref, tabp_ref, loc_hbm, pw_hbm, tm, loc_s, pw_s, sem)
        make(lambda rb, rs, cs: tm[rs, cs])

    keep = lax.broadcasted_iota(I32, e_ref.shape, 0) < left
    e = jnp.where(keep, e_ref[...], jnp.zeros((), BF16))
    du_ref[...] += lax.dot_general(g_ref[...], e, (((0,), (0,)), ((), ())), preferred_element_type=F32)


def du_call(scal, cnt, z, c, emb, tables, half):
    tabr, tabp, loc, pw = tables
    width, dim = z.shape[1], emb.shape[1]
    nb = half // VB1
    trows = VB1 // 128 * 8
    anyspace = pl.BlockSpec(memory_space=pl.ANY)
    return pl.pallas_call(
        du_kernel,
        out_shape=(
            jax.ShapeDtypeStruct((width, dim), F32),
            jax.ShapeDtypeStruct((half, width), BF16),
            jax.ShapeDtypeStruct((8, width), F32),
        ),
        grid_spec=pltpu.PrefetchScalarGridSpec(
            num_scalar_prefetch=2,
            grid=(nb,),
            in_specs=[
                pl.BlockSpec((VB1, width), lambda i, s, n: (i, 0)),
                pl.BlockSpec((1, width), lambda i, s, n: (0, 0)),
                pl.BlockSpec((VB1, dim), lambda i, s, n: (s[3] * nb + i, 0)),
                pl.BlockSpec((trows, width), lambda i, s, n: (i, 0)),
                pl.BlockSpec((trows, width), lambda i, s, n: (i, 0)),
                anyspace,
                anyspace,
            ],
            out_specs=(
                pl.BlockSpec((width, dim), lambda i, s, n: (0, 0)),
                pl.BlockSpec((VB1, width), lambda i, s, n: (i, 0)),
                pl.BlockSpec((8, width), lambda i, s, n: (0, 0)),
            ),
            scratch_shapes=[
                pltpu.VMEM((VB1, width), F32),
                pltpu.VMEM((loc.shape[0], 128), I32),
                pltpu.VMEM((loc.shape[0], 128), F32),
                pltpu.SemaphoreType.DMA((2,)),
            ],
        ),
        compiler_params=params(dimension_semantics=('arbitrary',)),
        cost_estimate=cost(2.0 * half * width * dim, half * dim * 2 + half * width * 6 + width * dim * 4, half * width),
        name='grad_u',
    )(scal, cnt, z, c, emb, tabr, tabp, loc, pw)


def de_kernel(b0, ny, aliased, sc_ref, cnt_ref, *refs):
    y_refs = refs[:ny]
    (scale_ref, z_ref, c_ref, gown_ref, tabr_ref, tabp_ref, loc_hbm, pw_hbm) = refs[ny:ny + 8]
    rest = refs[ny + 8 + (1 if aliased else 0):]
    out_ref, part_ref, u_ref, g_ref, tm, loc_s, pw_s, sem = rest
    i = pl.program_id(0)
    core = sc_ref[3]
    vb, width = z_ref.shape
    mine = gown_ref.shape[1]
    cols = out_ref.shape[1]
    nrb = vb // 128

    @pl.when(i == 0)
    def _():
        for a, y_ref in enumerate(y_refs):
            n = y_ref.shape[0]
            for k in range(2):
                src = pl.multiple_of((core if k == 0 else 1 - core) * cols, cols)
                u = y_ref[:, pl.ds(src, cols)] * scale_ref[:, pl.ds(src, cols)]
                u_ref[a * n:(a + 1) * n, k * cols:(k + 1) * cols] = u.astype(BF16)

    slots = most_slots(cnt_ref, (b0 + i) * nrb, nrb)

    def make(teacher):
        for cs0 in range(0, width, 256):
            cs = slice(cs0, cs0 + 256)
            for rb in range(nrb):
                rs = slice(rb * 128, (rb + 1) * 128)
                g = jnp.exp(z_ref[rs, cs] - c_ref[:, cs]) - teacher(rb, rs, cs)
                g_ref[rs, cs] = g.astype(BF16)

    @pl.when(slots <= FAST)
    def _():
        make(lambda rb, rs, cs: teacher_fast(tabr_ref, tabp_ref, rb, cs, 256))

    @pl.when(slots > FAST)
    def _():
        fill_teacher(cnt_ref, (b0 + i) * nrb, nrb, tabr_ref, tabp_ref, loc_hbm, pw_hbm, tm, loc_s, pw_s, sem)
        make(lambda rb, rs, cs: tm[rs, cs])

    acc = jnp.dot(gown_ref[...], u_ref[0:mine, :], preferred_element_type=F32)
    acc = acc + jnp.dot(g_ref[...], u_ref[mine:, :], preferred_element_type=F32)
    out_ref[...] = acc[:, :cols]
    part_ref[...] = acc[:, cols:]


def de_call(scal, cnt, y_all, xs, scale, z, c, gown, tables, half, vocab, b0, nb, prev):
    tabr, tabp, loc, pw = tables
    width, dim = z.shape[1], y_all.shape[1]
    mine = gown.shape[1]
    ccols = dim // xs
    cols = ccols // 2
    tot = half // VB
    trows = VB // 128 * 8
    anyspace = pl.BlockSpec(memory_space=pl.ANY)
    y_specs = [pl.BlockSpec((mine, ccols), functools.partial(lambda j, i, s, n: (lax.rem(s[2] + j, xs), s[2]), j))
               for j in range(xs)]
    in_specs = y_specs + [
        pl.BlockSpec((1, ccols), lambda i, s, n: (0, s[2])),
        pl.BlockSpec((VB, width), lambda i, s, n: (b0 + i, 0)),
        pl.BlockSpec((1, width), lambda i, s, n: (0, 0)),
        pl.BlockSpec((VB, mine), lambda i, s, n: (b0 + i, 0)),
        pl.BlockSpec((trows, width), lambda i, s, n: (b0 + i, 0)),
        pl.BlockSpec((trows, width), lambda i, s, n: (b0 + i, 0)),
        anyspace,
        anyspace,
    ]
    args = [y_all] * xs + [scale, z, c, gown, tabr, tabp, loc, pw]
    aliases = {}
    if prev is not None:
        aliases = {2 + len(args): 0}
        args.append(prev)
        in_specs.append(anyspace)
    return pl.pallas_call(
        functools.partial(de_kernel, b0, xs, prev is not None),
        out_shape=(jax.ShapeDtypeStruct((vocab, cols), F32), jax.ShapeDtypeStruct((nb * VB, cols), F32)),
        grid_spec=pltpu.PrefetchScalarGridSpec(
            num_scalar_prefetch=2,
            grid=(nb,),
            in_specs=in_specs,
            out_specs=(
                pl.BlockSpec((VB, cols), lambda i, s, n: (s[3] * tot + b0 + i, 0)),
                pl.BlockSpec((VB, cols), lambda i, s, n: (i, 0)),
            ),
            scratch_shapes=[
                pltpu.VMEM((width + mine, ccols), BF16),
                pltpu.VMEM((VB, width), BF16),
                pltpu.VMEM((VB, width), F32),
                pltpu.VMEM((loc.shape[0], 128), I32),
                pltpu.VMEM((loc.shape[0], 128), F32),
                pltpu.SemaphoreType.DMA((2,)),
            ],
        ),
        input_output_aliases=aliases,
        compiler_params=params(dimension_semantics=('arbitrary',)),
        cost_estimate=cost(3.0 * nb * VB * (width + mine) * ccols, nb * VB * (width * 4 + mine * 2 + ccols * 4), nb * VB * width),
    )(scal, cnt, *args)


def place_kernel(sc_ref, recv_ref, prev_ref, out_ref):
    out_ref[...] = recv_ref[...]


def place(scal, recv, out, half, row0):
    cols = out.shape[1]
    step = min(1024, recv.shape[0])
    return pl.pallas_call(
        place_kernel,
        out_shape=jax.ShapeDtypeStruct(out.shape, F32),
        grid_spec=pltpu.PrefetchScalarGridSpec(
            num_scalar_prefetch=1,
            grid=(recv.shape[0] // step,),
            in_specs=[pl.BlockSpec((step, cols), lambda i, s: (i, 0)), pl.BlockSpec(memory_space=pl.ANY)],
            out_specs=pl.BlockSpec((step, cols), lambda i, s: ((1 - s[3]) * (half // step) + row0 // step + i, 0)),
        ),
        input_output_aliases={2: 0},
        compiler_params=params(),
        cost_estimate=cost(1e8, recv.size * 8),
    )(scal, recv, out)


def solution(mesh):
    tps = mesh.shape['tp']
    xs = mesh.shape['dp'] // 2
    grid = Mesh(np.asarray(mesh.devices).reshape(tps, xs, 2), ('tp', 'x', 'core'))
    swap = [(0, 1), (1, 0)]
    everyone = ('x', 'core', 'tp')

    def local_head(hidden, embedding, norm_weight, teach_ids, teach_prob, tok_mask):
        vocab, dim = embedding.shape
        tok = hidden.shape[0]
        chip = 2 * tok
        top = teach_ids.shape[1]
        t, x, c = lax.axis_index('tp'), lax.axis_index('x'), lax.axis_index('core')
        half = -(-vocab // (2 * VB1)) * VB1
        nblk = half // 128
        part = tok // tps
        rows = jnp.where(c == 0, half, vocab - half)
        scal = jnp.stack([t * vocab + c * half, rows, x, c]).astype(I32)
        scale = (1.0 + norm_weight)[None, :]

        h_f32 = hidden.astype(F32)
        inv_rms = lax.rsqrt(jnp.mean(h_f32 * h_f32, axis=1, keepdims=True) + EPS_NORM)
        normed = h_f32 * inv_rms
        my_normed = lax.optimization_barrier(lax.dynamic_slice(normed, (t * part, 0), (part, dim)))
        y_all = lax.all_gather(my_normed, everyone, axis=0, tiled=True)
        y_part = lax.ppermute(normed, 'core', swap)
        lists = sort_lists(teach_ids, teach_prob, tok_mask)
        lists_part = lax.ppermute(lists, 'core', swap)
        lrows = 2 * top // tps
        lists_all = lax.all_gather(lax.dynamic_slice(lists, (t * lrows, 0), (lrows, tok)), everyone, axis=0, tiled=True)

        whole = pl.BlockSpec((tok, dim), lambda i, s: (0, 0))
        z0, m0, s0 = forward(scal, [normed, y_part], [whole, whole], scale, embedding, half, chip, True)
        chip_lists = jnp.where(c == 0, jnp.concatenate([lists, lists_part]), jnp.concatenate([lists_part, lists]))
        mask0 = (chip_lists.reshape(2, 2 * top, tok)[:, 0, :] > 0).astype(F32).reshape(1, chip)
        count = jnp.broadcast_to(jnp.sum(mask0), (1, 128))
        lse0, total = stats(m0, s0, count, tps, xs, 0)
        total = total[0, 0]

        def shift(lse, mask):
            weight = mask / total
            return weight, jnp.where(mask > 0, lse.reshape(1, -1) - jnp.log(weight), BIG)

        w0, c0 = shift(lse0, mask0)
        *tab0, cnt0, loc0, pw0 = expand(scal, chip_lists, w0, nblk, lambda g, s: (g // (tok // 128), g % (tok // 128)),
                                        chip // 128)
        cnt0 = jnp.max(cnt0.reshape(nblk, -1), axis=1)
        du, g0, tz = du_call(scal, cnt0, z0, c0, embedding, (*tab0, loc0, pw0), half)
        du_sum = lax.psum_scatter(du, ('core', 'tp'), scatter_dimension=0, tiled=True)

        y_specs = [pl.BlockSpec((chip, dim), functools.partial(lambda j, i, s: (lax.rem(s[2] + j, xs), 0), j))
                   for j in range(1, xs)]
        z1, m1, s1 = forward(scal, [y_all] * (xs - 1), y_specs, scale, embedding, half, (xs - 1) * chip, False)
        lse1, _ = stats(m1, s1, count, tps, xs, 1)
        signs = (lists_all.reshape(xs, 2, 2 * top, tok)[:, :, 0, :] > 0).astype(F32).reshape(xs, chip)
        order = lax.rem(x + jnp.arange(1, xs), xs)
        mask1 = signs[order].reshape(1, -1)
        w1, c1 = shift(lse1, mask1)
        tg = tok // 128

        def rest_map(g, s):
            return (lax.rem(s[2] + 1 + g // (2 * tg), xs) * 2 + lax.rem(g // tg, 2), lax.rem(g, tg))

        *tab1, cnt1, loc1, pw1 = expand(scal, lists_all, w1, nblk, rest_map, (xs - 1) * chip // 128)
        cnt1 = jnp.max(cnt1.reshape(nblk, -1), axis=1)

        d_normed = du_sum * scale
        d_rest = d_normed - my_normed * jnp.mean(d_normed * my_normed, axis=1, keepdims=True)
        d_all = lax.all_gather(d_rest, 'tp', axis=0, tiled=True)
        grad_hidden = (inv_rms * d_all).astype(BF16)
        tail = jnp.concatenate([jnp.sum(du_sum * my_normed, axis=0), jnp.broadcast_to(jnp.sum(tz), (128,))])
        tails = lax.all_gather(tail[None, :], everyone, axis=0, tiled=True)
        sums = jnp.sum(tails, axis=0)
        grad_norm = sums[:dim]
        log_sum = jnp.sum(w0.reshape(-1) * lse0.reshape(-1)) + jnp.sum(w1.reshape(-1) * lse1.reshape(-1))
        loss_mean = log_sum - sums[dim]

        tables = (*tab1, loc1, pw1)
        nb = half // VB
        n0 = nb // 2
        out, send0 = de_call(scal, cnt1, y_all, xs, scale, z1, c1, g0, tables, half, vocab, 0, n0, None)
        recv0 = lax.ppermute(send0, 'core', swap)
        out, send1 = de_call(scal, cnt1, y_all, xs, scale, z1, c1, g0, tables, half, vocab, n0, nb - n0, out)
        recv1 = lax.ppermute(send1, 'core', swap)
        out = place(scal, recv0, out, half, 0)
        out = place(scal, recv1, out, half, n0 * VB)
        return loss_mean, grad_hidden, out, grad_norm

    tokens = ('x', 'core')
    return jax.shard_map(
        local_head,
        mesh=grid,
        in_specs=(P(tokens, None), P('tp', None), P(None), P(tokens, None), P(tokens, None), P(tokens)),
        out_specs=(P(), P(tokens, None), P('tp', tokens), P(None)),
        check_vma=False,
    )
```

```python
import functools

import jax
import jax.numpy as jnp
import numpy as np
from jax import lax
from jax.experimental import pallas as pl
from jax.experimental.pallas import tpu as pltpu
from jax.sharding import Mesh
from jax.sharding import PartitionSpec as P


EPS_NORM = 1e-6
NEG = -1e30
BIG = 1e30
F32, BF16, I32 = jnp.float32, jnp.bfloat16, jnp.int32
LANES, SUB = 128, 8
SLOTS = 8
FAST = 2
TILE = 256
WIDE = 512
VMEM_LIMIT = 60 * 1024 * 1024
MESH = pl.DeviceIdType.MESH
VMEM = pl.BlockSpec(memory_space=pltpu.VMEM)
ANY = pl.BlockSpec(memory_space=pl.ANY)


def params(**kw):
    return pltpu.CompilerParams(vmem_limit_bytes=VMEM_LIMIT, **kw)


def cost(flops, nbytes, trans=0):
    return pl.CostEstimate(flops=int(flops), bytes_accessed=int(nbytes), transcendentals=int(trans))


def shape(rows, cols, dtype=F32):
    return jax.ShapeDtypeStruct((rows, cols), dtype)


def fixed(rows, cols):
    return pl.BlockSpec((rows, cols), lambda *a: (0, 0))


def by_row(rows, cols):
    return pl.BlockSpec((rows, cols), lambda i: (i, 0))


def sub8(a):
    return slice(SUB * a, SUB * a + SUB)


def iota(rows, cols, axis=0):
    return lax.broadcasted_iota(I32, (rows, cols), axis)


def at(start, size):
    return pl.ds(pl.multiple_of(start, size), size)


def core_rows(vocab, half):
    return jnp.where(lax.axis_index('core') == 0, half, vocab - half)


def sort_kernel(vocab, whole, ids_ref, pt_ref, mask_ref, out_ref):
    n = ids_ref.shape[1]
    sub = iota(SUB, LANES)
    nv = n // SUB
    base = lax.axis_index('tp') * vocab
    for g in range(ids_ref.shape[0] // LANES):
        cols = slice(g * LANES, (g + 1) * LANES)
        order = ids_ref[cols, :] - base
        key = (jnp.where(order < 0, order + whole, order) + 1).astype(F32).T
        prob = pt_ref[cols, :].T
        k = [key[sub8(a), :] for a in range(nv)]
        p = [prob[sub8(a), :] for a in range(nv)]
        size = 2
        while size <= n:
            j = size // 2
            while j:
                if j >= SUB:
                    for a in range(nv):
                        if (SUB * a) & j:
                            continue
                        b = a + j // SUB
                        up = ((SUB * a) & size) == 0
                        swap = k[a] > k[b] if up else k[a] < k[b]
                        lo, hi = jnp.minimum(k[a], k[b]), jnp.maximum(k[a], k[b])
                        k[a], k[b] = (lo, hi) if up else (hi, lo)
                        p[a], p[b] = jnp.where(swap, p[b], p[a]), jnp.where(swap, p[a], p[b])
                else:
                    low = (sub & j) == 0
                    for a in range(nv):
                        if size >= SUB:
                            want_min = low if ((SUB * a) & size) == 0 else (sub & j) != 0
                        else:
                            want_min = low == ((sub & size) == 0)
                        ka = jnp.where(low, pltpu.roll(k[a], SUB - j, 0), pltpu.roll(k[a], j, 0))
                        pa = jnp.where(low, pltpu.roll(p[a], SUB - j, 0), pltpu.roll(p[a], j, 0))
                        new = jnp.where(want_min, jnp.minimum(k[a], ka), jnp.maximum(k[a], ka))
                        p[a] = jnp.where(new == ka, pa, p[a])
                        k[a] = new
                j //= 2
            size *= 2
        sign = jnp.where(mask_ref[:, cols] > 0, 1.0, -1.0)
        for a in range(nv):
            out_ref[sub8(a), cols] = k[a] * sign
            out_ref[sub8(nv + a), cols] = p[a]


def sort_lists(ids, prob, mask, vocab, whole):
    tokens, top = ids.shape
    return pl.pallas_call(
        functools.partial(sort_kernel, vocab, whole),
        out_shape=shape(2 * top, tokens),
        in_specs=[VMEM] * 3,
        out_specs=VMEM,
        compiler_params=params(),
        cost_estimate=cost(4e9, tokens * top * 16),
        name='sort_lists',
    )(ids, prob, mask[None, :])


def roll_all(x, op):
    for sh in (4, 2, 1):
        x = op(x, pltpu.roll(x, sh, 0))
    return x


def expand_kernel(vocab, half, plan, *refs):
    lists, (w_ref, tabr_ref, tabp_ref, cnt_ref, loc_ref, pw_ref, src) = refs[:-7], refs[-7:]
    g = pl.program_id(0)
    core = lax.axis_index('core')
    rows = core_rows(vocab, half)
    top = src.shape[0] // 2
    nq = top // SUB
    nblk = half // LANES
    sub = iota(SUB, LANES)

    which = plan(g, core)
    for a, ref in enumerate(lists):
        @pl.when(which == a)
        def _():
            src[...] = ref[...]

    w = w_ref[...]
    over = jnp.zeros((SUB, LANES), I32)
    used = jnp.zeros((SUB, LANES), I32)
    first = jnp.full((SUB, LANES), nq, I32)
    prev = None
    for q in range(nq):
        order = jnp.abs(src[sub8(q), :]).astype(I32) - 1 - core * half
        ok = (order >= 0) & (order < rows)
        loc = jnp.where(ok, order, -1)
        loc_ref[sub8(q), :] = loc
        pw_ref[sub8(q), :] = src[sub8(nq + q), :] * w
        used = jnp.where(ok, q + 1, used)
        first = jnp.minimum(first, jnp.where(ok, q, nq))
        blk = loc >> 7
        if prev is not None:
            over = jnp.where((blk == prev) & ok, 1, over)
        prev = blk
    over = roll_all(over, jnp.maximum)
    lo, hi = jnp.min(first), jnp.max(used)

    @pl.when(g == 0)
    def _():
        cnt_ref[...] = jnp.zeros(cnt_ref.shape, I32)

    def body(bt, carry):
        b0 = bt * SUB

        def scan(q, acc):
            accc, accp = list(acc[0]), list(acc[1])
            here = at(q * SUB, SUB)
            loc = loc_ref[here, :]
            blk = (loc >> 7) - b0
            code = (sub + SUB * q) * LANES + (loc & (LANES - 1))
            p = pw_ref[here, :]
            for i in range(SUB):
                m = blk == i
                accc[i] = jnp.where(m, code, accc[i])
                accp[i] = jnp.where(m, p, accp[i])
            return tuple(accc), tuple(accp)

        empty = ((jnp.full((SUB, LANES), -1, I32),) * SUB, (jnp.zeros((SUB, LANES), F32),) * SUB)
        accc, accp = lax.fori_loop(lo, hi, scan, empty)
        most = jnp.zeros((SUB, LANES), I32)
        for i in range(SUB):
            code, p = accc[i], accp[i]
            head = roll_all(jnp.where(code >= 0, code, top * LANES), jnp.minimum)
            start = (head >> 7) & (SUB - 1)
            for sh in (1, 2, 4):
                move = (start & sh) != 0
                code = jnp.where(move, pltpu.roll(code, SUB - sh, 0), code)
                p = jnp.where(move, pltpu.roll(p, SUB - sh, 0), p)
            full = roll_all(jnp.where(code >= 0, sub + 1, 0), jnp.maximum)
            most = jnp.where(sub == i, full, most)
            row = at((b0 + i) * SUB, SUB)
            tabr_ref[row, :] = jnp.where(code >= 0, code & (LANES - 1), -1)
            tabp_ref[row, :] = p
        most = jnp.where(over > 0, SLOTS + 1, most)
        tile = at(b0, SUB)
        cnt_ref[tile, :] = jnp.maximum(cnt_ref[tile, :], most)
        return carry

    lax.fori_loop(0, nblk // SUB, body, 0)


def expand_call(lists, plan, lane_block, weight, vocab, half):
    top = lists[0].shape[0] // 2
    groups = weight.shape[1] // LANES
    nblk = half // LANES
    width = groups * LANES

    def spec(rows):
        return pl.BlockSpec((rows, LANES), lambda g: (0, g))

    tabr, tabp, cnt, loc, pw = pl.pallas_call(
        functools.partial(expand_kernel, vocab, half, plan),
        out_shape=(shape(nblk * SLOTS, width, I32), shape(nblk * SLOTS, width), shape(nblk, LANES, I32),
                   shape(top, width, I32), shape(top, width)),
        grid=(groups,),
        in_specs=[pl.BlockSpec((2 * top, LANES), lambda g: (0, lane_block(g)))] * len(lists) + [spec(1)],
        out_specs=(spec(nblk * SLOTS), spec(nblk * SLOTS), fixed(nblk, LANES), spec(top), spec(top)),
        scratch_shapes=[pltpu.VMEM((2 * top, LANES), F32)],
        compiler_params=params(),
        cost_estimate=cost(groups * 1e8, 4 * width * (4 * top + 2 * nblk * SLOTS)),
    )(*lists, weight)
    return (tabr, tabp, loc, pw), jnp.max(cnt, axis=1)


def tp_peer(j, tps):
    return {'tp': lax.rem(lax.axis_index('tp') + j, tps)}


def reduce_start(tps, du_ref, recv, ssem, rsem):
    rows = recv.shape[1]
    t = lax.axis_index('tp')
    barrier = pltpu.get_barrier_semaphore()

    def hello(j, carry):
        pl.semaphore_signal(barrier, inc=1, device_id=tp_peer(j, tps), device_id_type=MESH)
        return carry

    lax.fori_loop(1, tps, hello, 0)
    pl.semaphore_wait(barrier, tps - 1)
    pltpu.make_async_copy(du_ref.at[at(t * rows, rows), :], recv.at[0], rsem.at[0]).start()

    def start(j, carry):
        reduce_copy(j, tps, du_ref, recv, ssem, rsem).start()
        return carry

    lax.fori_loop(1, tps, start, 0)


def reduce_copy(j, tps, du_ref, recv, ssem, rsem):
    rows = recv.shape[1]
    peer = lax.rem(lax.axis_index('tp') + j, tps)
    return pltpu.make_async_remote_copy(
        src_ref=du_ref.at[at(peer * rows, rows), :], dst_ref=recv.at[j], send_sem=ssem.at[j], recv_sem=rsem.at[j],
        device_id={'tp': peer}, device_id_type=MESH)


def reduce_finish(tps, du_ref, y_ref, scale_ref, recv, ssem, rsem, rest_ref, dw_ref):
    rows = recv.shape[1]
    t = lax.axis_index('tp')
    pltpu.make_async_copy(du_ref.at[at(t * rows, rows), :], recv.at[0], rsem.at[0]).wait()

    def finish(j, carry):
        reduce_copy(j, tps, du_ref, recv, ssem, rsem).wait()
        return carry

    lax.fori_loop(1, tps, finish, 0)
    du = jnp.sum(recv[...], axis=0)
    y = y_ref[...]
    dy = du * scale_ref[...]
    rest_ref[...] = dy - y * jnp.mean(dy * y, axis=1, keepdims=True)
    dw_ref[...] = jnp.sum(du * y, axis=0, keepdims=True)


def fwd_kernel(vocab, half, bases, tps, *refs):
    ny = 2 * len(bases)
    y_refs, refs = refs[:ny], refs[ny:]
    scale_ref, e_ref = refs[:2]
    if tps:
        du_ref, ysl_ref, z_ref, m_ref, s_ref, u_ref, rest_ref, dw_ref, ut_ref, recv, ssem, rsem = refs[2:]
    else:
        z_ref, m_ref, s_ref, u_ref, ut_ref = refs[2:]
    i = pl.program_id(0)
    x, core = lax.axis_index('x'), lax.axis_index('core')
    rows = core_rows(vocab, half)
    cols = u_ref.shape[1] // 2

    @pl.when(i == 0)
    def _():
        if tps:
            reduce_start(tps, du_ref, recv, ssem, rsem)
        for a, y_ref in enumerate(y_refs):
            n = y_ref.shape[0]
            slot = core if a % 2 == 0 else 1 - core
            dest = at(bases[a // 2] + slot * n, n)
            ut_ref[:, dest] = (y_ref[...] * scale_ref[...]).astype(BF16).T
            for k in range(2):
                mine = at((2 * x + (core if k == 0 else 1 - core)) * cols, cols)
                u_ref[dest, k * cols:(k + 1) * cols] = (y_ref[:, mine] * scale_ref[:, mine]).astype(BF16)
        m_ref[...] = jnp.full(m_ref.shape, NEG, F32)
        s_ref[...] = jnp.zeros(s_ref.shape, F32)

    vb = e_ref.shape[0]
    left = rows - i * vb
    for r0 in range(0, vb, TILE):
        rs = slice(r0, r0 + TILE)
        keep = iota(TILE, WIDE) < left - r0
        for c0 in range(0, ut_ref.shape[1], WIDE):
            cs = slice(c0, c0 + WIDE)
            z = jnp.dot(e_ref[rs, :], ut_ref[:, cs], preferred_element_type=F32)
            z = jnp.where(keep, z, NEG)
            z_ref[rs, cs] = z
            z3 = z.reshape(TILE // SUB, SUB, WIDE)
            old = m_ref[:, cs]
            new = jnp.maximum(old, jnp.max(z3, axis=0))
            m_ref[:, cs] = new
            s_ref[:, cs] = s_ref[:, cs] * jnp.exp(old - new) + jnp.sum(jnp.exp(z3 - new[None]), axis=0)

    if tps:
        @pl.when(i == pl.num_programs(0) - 1)
        def _():
            reduce_finish(tps, du_ref, ysl_ref, scale_ref, recv, ssem, rsem, rest_ref, dw_ref)


def forward(ys, scale, emb, half, vb, du=None, ysl=None, tps=0):
    vocab, dim = emb.shape
    nb = half // vb
    bases, width = [], 0
    for y in ys[::2]:
        bases.append(width)
        width += 2 * y.shape[0]
    ccols = dim // 4
    in_specs = [fixed(*y.shape) for y in ys]
    in_specs += [fixed(1, dim), pl.BlockSpec((vb, dim), lambda i: (lax.axis_index('core') * nb + i, 0))]
    args = [*ys, scale, emb]
    out_shape = [shape(half, width), shape(SUB, width), shape(SUB, width), shape(width, ccols, BF16)]
    out_specs = [by_row(vb, width), fixed(SUB, width), fixed(SUB, width), fixed(width, ccols)]
    scratch = [pltpu.VMEM((dim, width), BF16)]
    more = {}
    if tps:
        part = ysl.shape[0]
        in_specs += [ANY, fixed(part, dim)]
        args += [du, ysl]
        out_shape += [shape(part, dim), shape(1, dim)]
        out_specs += [fixed(part, dim), fixed(1, dim)]
        scratch += [pltpu.VMEM((tps, part, dim), F32), pltpu.SemaphoreType.DMA((tps,)), pltpu.SemaphoreType.DMA((tps,))]
        more = dict(collective_id=3, has_side_effects=True)
    return pl.pallas_call(
        functools.partial(fwd_kernel, vocab, half, tuple(bases), tps),
        out_shape=out_shape,
        grid=(nb,),
        in_specs=in_specs,
        out_specs=out_specs,
        scratch_shapes=scratch,
        compiler_params=params(dimension_semantics=('arbitrary',), **more),
        cost_estimate=cost(2.0 * half * width * dim, half * dim * 2 + half * width * 4 + width * dim * 4, half * width),
    )(*args)


def pieces(x):
    return [x[:, g * LANES:(g + 1) * LANES] for g in range(x.shape[1] // LANES)]


def put_rows(ref, base, x):
    for g, piece in enumerate(pieces(x)):
        ref[base + g:base + g + 1, :] = piece


def stats_kernel(tps, xs, order, own, *refs):
    nlist = 2 * len(order)
    lists, refs = refs[:nlist], refs[nlist:]
    nstat = 2 if own else 4
    stat, refs = refs[:nstat], refs[nstat:]
    nadd = 0 if own else 3
    adds, refs = refs[:nadd], refs[nadd:]
    c_ref, w_ref, loss_ref, sums_ref, send, recv, xsend, xrecv, tsend, trecv, ssem, rsem, xssem, xrsem, tssem, trsem = refs
    t, x, core = lax.axis_index('tp'), lax.axis_index('x'), lax.axis_index('core')
    me = t * 2 + core
    peers = tps * 2
    near = xs * 2
    here = x * 2 + core
    gr = send.shape[0] // 2

    base = 0
    send[...] = jnp.zeros(send.shape, F32)
    for m_ref, s_ref in zip(stat[::2], stat[1::2]):
        m = jnp.max(m_ref[...], axis=0, keepdims=True)
        s = jnp.sum(s_ref[...] * jnp.exp(m_ref[...] - m), axis=0, keepdims=True)
        put_rows(send, base, m)
        put_rows(send, gr + base, s)
        base += m.shape[1] // LANES
    masks = []
    for (chip, lanes) in order_list(order):
        a, b = (ref[0:1, lanes] for ref in lists[2 * chip:2 * chip + 2])
        masks += [jnp.where(core == 0, a, b), jnp.where(core == 0, b, a)]
    mask = (jnp.concatenate(masks, axis=1) > 0).astype(F32)
    xsend[...] = jnp.zeros(xsend.shape, F32)
    if own:
        put_rows(xsend, 0, mask)
    else:
        put_rows(xsend, 0, adds[0][...])
        tz = jnp.sum(adds[1][...], axis=0, keepdims=True)
        xsend[xsend.shape[0] - SUB:xsend.shape[0] - SUB + 1, :] = functools.reduce(jnp.add, pieces(tz))

    barrier = pltpu.get_barrier_semaphore()

    def peer(j):
        r = lax.rem(me + j, peers)
        return {'tp': r // 2, 'core': lax.rem(r, 2)}

    def xpeer(j):
        r = lax.rem(here + j, near)
        return {'x': r // 2, 'core': lax.rem(r, 2)}

    def signal(to):
        def run(j, carry):
            pl.semaphore_signal(barrier, inc=1, device_id=to(j), device_id_type=MESH)
            return carry

        return run

    lax.fori_loop(1, peers, signal(peer), 0)
    lax.fori_loop(1, near, signal(xpeer), 0)
    pl.semaphore_wait(barrier, peers + near - 2)

    def copies(src, dst, s, r, to):
        def make(j):
            return pltpu.make_async_remote_copy(
                src_ref=src, dst_ref=dst.at[j], send_sem=s.at[j], recv_sem=r.at[j], device_id=to(j), device_id_type=MESH)

        def start(j, carry):
            make(j).start()
            return carry

        def wait(j, carry):
            make(j).wait()
            return carry

        return start, wait

    start, wait = copies(send, recv, ssem, rsem, peer)
    xstart, xwait = copies(xsend, xrecv, xssem, xrsem, xpeer)
    lax.fori_loop(1, near, xstart, 0)
    lax.fori_loop(1, peers, start, 0)
    lax.fori_loop(1, near, xwait, 0)
    total = xsend[...] + jnp.sum(xrecv[1:], axis=0)
    if not own:
        tsend[...] = total
        tstart, twait = copies(tsend, trecv, tssem, trsem, functools.partial(tp_peer, tps=tps))
        lax.fori_loop(1, tps, tstart, 0)
    lax.fori_loop(1, peers, wait, 0)
    mine, theirs = send[0:gr, :], recv[1:, 0:gr, :]
    best = jnp.maximum(mine, jnp.max(theirs, axis=0))
    acc = send[gr:, :] * jnp.exp(mine - best) + jnp.sum(recv[1:, gr:, :] * jnp.exp(theirs - best[None]), axis=0)
    lse = best + jnp.log(acc)
    lse = jnp.concatenate([lse[g:g + 1, :] for g in range(mask.shape[1] // LANES)], axis=1)
    if own:
        count = jnp.broadcast_to(jnp.sum(total, keepdims=True) / 2, (1, LANES))
        sums_ref[...] = count
    else:
        count = adds[2][...]
    w = mask / count[:, 0:1]
    w_ref[...] = w
    c_ref[...] = jnp.where(mask > 0, lse - jnp.log(w), BIG)
    loss_ref[...] = functools.reduce(jnp.add, pieces(w * lse))
    if not own:
        lax.fori_loop(1, tps, twait, 0)
        sums_ref[...] = tsend[...] + jnp.sum(trecv[1:], axis=0)


def order_list(order):
    return [(chip, lanes) for chip, cuts in enumerate(order) for lanes in cuts]


def stats(lists, order, stat, adds, tps, xs, cid):
    own = not adds
    width = sum(m.shape[1] for m in stat[::2])
    tok = lists[0].shape[1]
    gr = -(-width // (LANES * SUB)) * SUB
    xr = SUB if own else adds[0].shape[1] // LANES + SUB
    dma = pltpu.SemaphoreType.DMA
    return pl.pallas_call(
        functools.partial(stats_kernel, tps, xs, order, own),
        out_shape=(shape(1, width), shape(1, width), shape(1, LANES), shape(1 if own else xr, LANES)),
        grid=(1,),
        in_specs=[fixed(SUB, tok)] * len(lists) + [fixed(*a.shape) for a in (*stat, *adds)],
        out_specs=(fixed(1, width), fixed(1, width), fixed(1, LANES), fixed(1 if own else xr, LANES)),
        scratch_shapes=[
            pltpu.VMEM((2 * gr, LANES), F32),
            pltpu.VMEM((2 * tps, 2 * gr, LANES), F32),
            pltpu.VMEM((xr, LANES), F32),
            pltpu.VMEM((2 * xs, xr, LANES), F32),
            pltpu.VMEM((xr, LANES), F32),
            pltpu.VMEM((tps, xr, LANES), F32),
            dma((2 * tps,)), dma((2 * tps,)), dma((2 * xs,)), dma((2 * xs,)), dma((tps,)), dma((tps,)),
        ],
        compiler_params=params(collective_id=cid, has_side_effects=True),
        cost_estimate=cost(2e9, 1 << 16),
    )(*lists, *stat, *adds)


def fill_teacher(cnt_ref, first, nrb, tabr_ref, tabp_ref, loc_hbm, pw_hbm, tm, loc_s, pw_s, sem):
    width = tm.shape[1]
    rows = iota(LANES, LANES)
    zero = jnp.zeros((LANES, LANES), F32)

    def pick(row, val, t):
        for s in range(SUB):
            t = jnp.where(rows == row[s:s + 1, :], val[s:s + 1, :], t)
        return t

    for rb in range(nrb):
        n = cnt_ref[first + rb]
        rs = slice(rb * LANES, (rb + 1) * LANES)

        def tile(g, carry):
            lanes = at(g * LANES, LANES)

            @pl.when(n <= SLOTS)
            def _():
                tm[rs, lanes] = pick(tabr_ref[sub8(rb), lanes], tabp_ref[sub8(rb), lanes], zero)

            @pl.when(n > SLOTS)
            def _():
                a = pltpu.make_async_copy(loc_hbm.at[:, lanes], loc_s, sem.at[0])
                b = pltpu.make_async_copy(pw_hbm.at[:, lanes], pw_s, sem.at[1])
                a.start()
                b.start()
                a.wait()
                b.wait()
                base = (first + rb) * LANES

                def entries(k, t):
                    here = at(k * SUB, SUB)
                    return pick(loc_s[here, :] - base, pw_s[here, :], t)

                tm[rs, lanes] = lax.fori_loop(0, loc_s.shape[0] // SUB, entries, zero)

            return carry

        lax.fori_loop(0, width // LANES, tile, 0)


def teacher_fast(tabr_ref, tabp_ref, rb, cs):
    rows = iota(LANES, TILE)
    t = jnp.zeros((LANES, TILE), F32)
    for s in range(SUB * rb, SUB * rb + FAST):
        t = jnp.where(rows == tabr_ref[s:s + 1, cs], tabp_ref[s:s + 1, cs], t)
    return t


def most_slots(cnt_ref, first, nrb):
    n = cnt_ref[first]
    for rb in range(1, nrb):
        n = jnp.maximum(n, cnt_ref[first + rb])
    return n


def fill_scratch(vb, width, top):
    return [pltpu.VMEM((vb, width), F32), pltpu.VMEM((top, LANES), I32), pltpu.VMEM((top, LANES), F32),
            pltpu.SemaphoreType.DMA((2,))]


def g_kernel(cnt_ref, z_ref, c_ref, tabr_ref, tabp_ref, loc_hbm, pw_hbm, g_ref, gt_ref, tz_ref, *fill):
    i = pl.program_id(0)
    vb, width = z_ref.shape
    nrb = vb // LANES

    @pl.when(i == 0)
    def _():
        tz_ref[...] = jnp.zeros(tz_ref.shape, F32)

    slots = most_slots(cnt_ref, i * nrb, nrb)

    def make(teacher):
        for c0 in range(0, width, TILE):
            cs = slice(c0, c0 + TILE)
            tz = jnp.zeros((SUB, TILE), F32)
            for rb in range(nrb):
                rs = slice(rb * LANES, (rb + 1) * LANES)
                z = z_ref[rs, cs]
                t = teacher(rb, rs, cs)
                g = (jnp.exp(z - c_ref[:, cs]) - t).astype(BF16)
                g_ref[rs, cs] = g
                gt_ref[cs, rs] = g.T
                tz = tz + jnp.sum((t * z).reshape(LANES // SUB, SUB, TILE), axis=0)
            tz_ref[:, cs] += tz

    @pl.when(slots <= FAST)
    def _():
        make(lambda rb, rs, cs: teacher_fast(tabr_ref, tabp_ref, rb, cs))

    @pl.when(slots > FAST)
    def _():
        fill_teacher(cnt_ref, i * nrb, nrb, tabr_ref, tabp_ref, loc_hbm, pw_hbm, *fill)
        make(lambda rb, rs, cs: fill[0][rs, cs])


def g_own(cnt, z, c, tables):
    half, width = z.shape
    vb = WIDE
    trows = vb // LANES * SLOTS

    def row(i, n):
        return (i, 0)

    return pl.pallas_call(
        g_kernel,
        out_shape=(shape(half, width, BF16), shape(width, half, BF16), shape(SUB, width)),
        grid_spec=pltpu.PrefetchScalarGridSpec(
            num_scalar_prefetch=1,
            grid=(half // vb,),
            in_specs=[pl.BlockSpec((vb, width), row), fixed(1, width), pl.BlockSpec((trows, width), row),
                      pl.BlockSpec((trows, width), row), ANY, ANY],
            out_specs=(pl.BlockSpec((vb, width), row), pl.BlockSpec((width, vb), lambda i, n: (0, i)), fixed(SUB, width)),
            scratch_shapes=fill_scratch(vb, width, tables[2].shape[0]),
        ),
        compiler_params=params(dimension_semantics=('arbitrary',)),
        cost_estimate=cost(4e9, half * width * 8, half * width),
        name='g_own',
    )(cnt, z, c, *tables)


def du_kernel(vocab, half, gt_ref, e_ref, out_ref, mine, send, recv, ssem, rsem):
    i = pl.program_id(0)
    core = lax.axis_index('core')
    rows = core_rows(vocab, half)
    tok = out_ref.shape[0]
    tiles = pl.num_programs(0) - 2
    cut = (vocab - half) // TILE * TILE

    @pl.when(i == 0)
    def _():
        barrier = pltpu.get_barrier_semaphore()
        pl.semaphore_signal(barrier, inc=1, device_id={'core': 1 - core}, device_id_type=MESH)
        pl.semaphore_wait(barrier, 1)

    def copy(k):
        return pltpu.make_async_remote_copy(
            src_ref=send.at[k], dst_ref=recv.at[k], send_sem=ssem.at[k], recv_sem=rsem.at[k],
            device_id={'core': 1 - core}, device_id_type=MESH)

    @pl.when((i >= 1) & (i <= tiles))
    def _():
        copy(i - 1).start()

    @pl.when(i < tiles)
    def _():
        tail = e_ref[cut:, :]
        tail = jnp.where(iota(*tail.shape) < rows - cut, tail, jnp.zeros((), BF16))

        def part(which):
            g = gt_ref[at(which * tok, tok), :]
            return (jnp.dot(g[:, :cut], e_ref[:cut, :], preferred_element_type=F32)
                    + jnp.dot(g[:, cut:], tail, preferred_element_type=F32))

        send[i] = part(1 - core)
        mine[i] = part(core)

    @pl.when(i >= 2)
    def _():
        copy(i - 2).wait()
        out_ref[...] = mine[i - 2] + recv[i - 2]


def du_call(gt, emb, half):
    vocab, dim = emb.shape
    tok = gt.shape[0] // 2
    tiles = dim // WIDE
    buf = pltpu.VMEM((tiles, tok, WIDE), F32)
    dma = pltpu.SemaphoreType.DMA((tiles,))
    return pl.pallas_call(
        functools.partial(du_kernel, vocab, half),
        out_shape=shape(tok, dim),
        grid=(tiles + 2,),
        in_specs=[fixed(*gt.shape),
                  pl.BlockSpec((half, WIDE), lambda i: (lax.axis_index('core'), jnp.minimum(i, tiles - 1)))],
        out_specs=pl.BlockSpec((tok, WIDE), lambda i: (0, jnp.maximum(i - 2, 0))),
        scratch_shapes=[buf, buf, buf, dma, dma],
        compiler_params=params(dimension_semantics=('arbitrary',), collective_id=2, has_side_effects=True),
        cost_estimate=cost(4.0 * half * tok * dim, half * dim * 2),
        name='grad_u',
    )(gt, emb)


def de_kernel(b0, refs_y, cnt_ref, *refs):
    u_refs, refs = refs[:refs_y], refs[refs_y:]
    zn_ref, zf_ref, gown_ref, c_ref, tabr_ref, tabp_ref, loc_hbm, pw_hbm = refs[:8]
    out_ref, part_ref, u_ref, g_ref, *fill = refs[-8:]
    i = pl.program_id(0)
    vb, mine = gown_ref.shape
    cols = out_ref.shape[1]
    nrb = vb // LANES
    first = (b0 + jnp.minimum(i, pl.num_programs(0) - 2)) * nrb

    @pl.when(i == 0)
    def _():
        base = 0
        for ref in u_refs:
            u_ref[base:base + ref.shape[0], :] = ref[...]
            base += ref.shape[0]

    def make(p, teacher):
        g_ref[p, :, 0:mine] = gown_ref[...]
        c0 = 0
        for z_ref in (zn_ref, zf_ref):
            for l0 in range(0, z_ref.shape[1], TILE):
                cs = slice(c0, c0 + TILE)
                for rb in range(nrb):
                    rs = slice(rb * LANES, (rb + 1) * LANES)
                    g = jnp.exp(z_ref[rs, l0:l0 + TILE] - c_ref[:, cs]) - teacher(rb, rs, cs)
                    g_ref[p, rs, mine + c0:mine + c0 + TILE] = g.astype(BF16)
                c0 += TILE

    for p in range(2):
        @pl.when(lax.rem(i, 2) == p)
        def _():
            make(p, lambda rb, rs, cs: teacher_fast(tabr_ref, tabp_ref, rb, cs))
            acc = jnp.dot(g_ref[1 - p], u_ref[...], preferred_element_type=F32)
            out_ref[...] = acc[:, :cols]
            part_ref[...] = acc[:, cols:]

    @pl.when(most_slots(cnt_ref, first, nrb) > FAST)
    def _():
        fill_teacher(cnt_ref, first, nrb, tabr_ref, tabp_ref, loc_hbm, pw_hbm, *fill)
        for p in range(2):
            @pl.when(lax.rem(i, 2) == p)
            def _():
                make(p, lambda rb, rs, cs: fill[0][rs, cs])


def de_call(cnt, us, zn, zf, gown, c, tables, vocab, b0, nb, prev):
    half, mine = gown.shape
    ccols = us[0].shape[1]
    cols = ccols // 2
    tot = half // TILE
    width = zn.shape[1] + zf.shape[1]
    trows = TILE // LANES * SLOTS

    def rows(cols_, height=TILE):
        return pl.BlockSpec((height, cols_), lambda i, n: (b0 + jnp.minimum(i, nb - 1), 0))

    in_specs = [fixed(*u.shape) for u in us]
    in_specs += [rows(zn.shape[1]), rows(zf.shape[1]), rows(mine), fixed(1, width), rows(width, trows), rows(width, trows),
                 ANY, ANY]
    args = [*us, zn, zf, gown, c, *tables]
    aliases = {}
    if prev is not None:
        aliases = {1 + len(args): 0}
        args.append(prev)
        in_specs.append(ANY)
    return pl.pallas_call(
        functools.partial(de_kernel, b0, len(us)),
        out_shape=(shape(vocab, cols), shape(nb * TILE, cols)),
        grid_spec=pltpu.PrefetchScalarGridSpec(
            num_scalar_prefetch=1,
            grid=(nb + 1,),
            in_specs=in_specs,
            out_specs=(
                pl.BlockSpec((TILE, cols), lambda i, n: (lax.axis_index('core') * tot + b0 + jnp.maximum(i - 1, 0), 0)),
                pl.BlockSpec((TILE, cols), lambda i, n: (jnp.maximum(i - 1, 0), 0)),
            ),
            scratch_shapes=[pltpu.VMEM((width + mine, ccols), BF16), pltpu.VMEM((2, TILE, width + mine), BF16),
                            *fill_scratch(TILE, width, tables[2].shape[0])],
        ),
        input_output_aliases=aliases,
        compiler_params=params(dimension_semantics=('arbitrary',)),
        cost_estimate=cost(3.0 * nb * TILE * (width + mine) * ccols, nb * TILE * (width * 4 + mine * 2 + ccols * 4),
                           nb * TILE * width),
    )(cnt, *args)


def place_kernel(recv_ref, prev_ref, out_ref):
    out_ref[...] = recv_ref[...]


def place(recv, out, half, row0):
    cols = out.shape[1]
    step = 2 * WIDE
    return pl.pallas_call(
        place_kernel,
        out_shape=shape(*out.shape),
        grid=(recv.shape[0] // step,),
        in_specs=[by_row(step, cols), ANY],
        out_specs=pl.BlockSpec(
            (step, cols), lambda i: ((1 - lax.axis_index('core')) * (half // step) + row0 // step + i, 0)),
        input_output_aliases={1: 0},
        compiler_params=params(),
        cost_estimate=cost(1e8, recv.size * 8),
    )(recv, out)


def dh_kernel(tps, *refs):
    parts, (inv_ref, out_ref) = refs[:tps], refs[tps:]
    t = lax.axis_index('tp')
    for j, ref in enumerate(parts):
        rows = ref.shape[0]
        here = at(lax.rem(t - j + tps, tps) * rows, rows)
        out_ref[here, :] = (inv_ref[here, :] * ref[...]).astype(BF16)


def dh_call(parts, inv):
    tps = len(parts)
    part, dim = parts[0].shape
    return pl.pallas_call(
        functools.partial(dh_kernel, tps),
        out_shape=shape(part * tps, dim, BF16),
        in_specs=[VMEM] * (tps + 1),
        out_specs=VMEM,
        compiler_params=params(),
        cost_estimate=cost(1e8, part * tps * dim * 6),
        name='grad_h',
    )(*parts, inv)


def solution(mesh):
    tps = mesh.shape['tp']
    xs = mesh.shape['dp'] // 2
    grid = Mesh(np.asarray(mesh.devices).reshape(tps, xs, 2), ('tp', 'x', 'core'))

    def shift(x, axis, by):
        n = grid.shape[axis]
        return lax.ppermute(x, axis, [(i, (i + by) % n) for i in range(n)])

    def both(x):
        return [x, shift(x, 'core', 1)]

    def local_head(hidden, embedding, norm_weight, teach_ids, teach_prob, tok_mask):
        vocab, dim = embedding.shape
        tok = hidden.shape[0]
        half = -(-vocab // (2 * WIDE)) * WIDE
        part = tok // tps
        cut = tok // 2
        scale = (1.0 + norm_weight)[None, :]

        h_f32 = hidden.astype(F32)
        inv_rms = lax.rsqrt(jnp.mean(h_f32 * h_f32, axis=1, keepdims=True) + EPS_NORM)
        normed = lax.optimization_barrier(h_f32 * inv_rms)
        left = shift(normed, 'x', 1)
        right = shift(normed, 'x', -1)
        y_own = both(normed)
        lists = sort_lists(teach_ids, teach_prob, tok_mask, vocab, vocab * tps)
        l_own = both(lists)

        z0, m0, s0, u0 = forward(y_own, scale, embedding, half, 2 * WIDE)
        full = slice(0, tok)
        lo, hi = slice(0, cut), slice(cut, tok)
        c0, w0, loss0, count = stats(l_own, ((full,),), (m0, s0), (), tps, xs, 0)
        tg = tok // LANES
        tab0, cnt0 = expand_call(l_own, lambda g, c: lax.rem(g // tg + c, 2), lambda g: lax.rem(g, tg),
                                 w0, vocab, half)
        g0, gt0, tz = g_own(cnt0, z0, c0, tab0)
        du = du_call(gt0, embedding, half)

        far0 = shift(left[:cut], 'x', 1)
        far1 = shift(right[cut:], 'x', -1)
        l_left = shift(lists, 'x', 1)
        l_right = shift(lists, 'x', -1)
        l_far = shift(l_left, 'x', 1)
        y_near = both(left) + both(right)
        y_far = both(far0) + both(far1)
        l_rest = both(l_left) + both(l_right) + both(l_far)
        my_normed = lax.dynamic_slice(normed, (lax.axis_index('tp') * part, 0), (part, dim))
        z1, m1, s1, u1, d_rest, dw = forward(y_near, scale, embedding, half, WIDE, du, my_normed, tps)
        d_parts = [d_rest] + [shift(d_rest, 'tp', j) for j in range(1, tps)]
        z2, m2, s2, u2 = forward(y_far, scale, embedding, half, 2 * WIDE)
        c1, w1, loss1, sums = stats(l_rest, ((full,), (full,), (lo, hi)), (m1, s1, m2, s2), (dw, tz, count),
                                    tps, xs, 1)

        def plan(g, c):
            far = g // (2 * tg) == 2
            swap = jnp.where(far, lax.rem(g, 2), lax.rem(g // tg, 2))
            return g // (2 * tg) * 2 + lax.rem(swap + c, 2)

        def lane_block(g):
            return jnp.where(g // (2 * tg) == 2, lax.rem(g // 2, tg), lax.rem(g, tg))

        tab1, cnt1 = expand_call(l_rest, plan, lane_block, w1, vocab, half)

        grad_norm = sums[:dim // LANES].reshape(dim)
        loss_mean = jnp.sum(loss0) + jnp.sum(loss1) - jnp.sum(sums[dim // LANES])

        us = [u0, u1, u2]
        nb = half // TILE
        n0 = nb // 2
        out, send0 = de_call(cnt1, us, z1, z2, g0, c1, tab1, vocab, 0, n0, None)
        recv0 = shift(send0, 'core', 1)
        out, send1 = de_call(cnt1, us, z1, z2, g0, c1, tab1, vocab, n0, nb - n0, out)
        recv1 = shift(send1, 'core', 1)
        grad_hidden = dh_call(d_parts, inv_rms)
        out = place(recv0, out, half, 0)
        out = place(recv1, out, half, n0 * TILE)
        return loss_mean, grad_hidden, out, grad_norm

    tokens = ('x', 'core')
    return jax.shard_map(
        local_head,
        mesh=grid,
        in_specs=(P(tokens, None), P('tp', None), P(None), P(tokens, None), P(tokens, None), P(tokens)),
        out_specs=(P(), P(tokens, None), P('tp', tokens), P(None)),
        check_vma=False,
    )
```

```python
import functools

import jax
import jax.numpy as jnp
import numpy as np
from jax import lax
from jax.experimental import pallas as pl
from jax.experimental.pallas import tpu as pltpu
from jax.sharding import Mesh
from jax.sharding import PartitionSpec as P


EPS_NORM = 1e-6
BIG = 1e30
NEG = -BIG
SMALL, LARGE = 1e8, 4e9
F32, BF16, I32 = jnp.float32, jnp.bfloat16, jnp.int32
LANES, SUB = 128, 8
ORDERED = ('arbitrary',)
SLOTS = 8
FAST = 2
TILE = 256
WIDE = 512
VMEM_LIMIT = 60 * 1024 * 1024
MESH = pl.DeviceIdType.MESH
VMEM = pl.BlockSpec(memory_space=pltpu.VMEM)
ANY = pl.BlockSpec(memory_space=pl.ANY)


def params(**kw):
    return pltpu.CompilerParams(vmem_limit_bytes=VMEM_LIMIT, **kw)


def cost(flops, nbytes, trans=0):
    return pl.CostEstimate(flops=int(flops), bytes_accessed=int(nbytes), transcendentals=int(trans))


def shape(rows, cols, dtype=F32):
    return jax.ShapeDtypeStruct((rows, cols), dtype)


def fixed(rows, cols):
    return pl.BlockSpec((rows, cols), lambda *a: (0, 0))


def one_row(cols):
    return fixed(1, cols)


def by_row(rows, cols):
    return pl.BlockSpec((rows, cols), lambda i: (i, 0))


def sub8(a):
    return slice(SUB * a, SUB * a + SUB)


def iota(rows, cols, axis=0):
    return lax.broadcasted_iota(I32, (rows, cols), axis)


def at(start, size):
    return pl.ds(pl.multiple_of(start, size), size)


def step_id():
    return pl.program_id(0)


def last_step():
    return pl.num_programs(0) - 1


def row_of(x):
    return (1, x.size)


def line(cols):
    return shape(1, cols)


def core_rows(vocab, half):
    return jnp.where(lax.axis_index('core') == 0, half, vocab - half)


class Links:
    def __init__(self, ssem, rsem):
        self.ssem, self.rsem, self.used = ssem, rsem, 0

    def copy(self, src, dst, to):
        k = self.used
        self.used += 1
        return pltpu.make_async_remote_copy(
            src_ref=src, dst_ref=dst, send_sem=self.ssem.at[k], recv_sem=self.rsem.at[k], device_id=to, device_id_type=MESH)


def start(copies):
    for c in copies:
        c.start()


def wait(copies):
    for c in copies:
        c.wait()


def hello(peers):
    for to in peers:
        pl.semaphore_signal(pltpu.get_barrier_semaphore(), inc=1, device_id=to, device_id_type=MESH)


def meet(peers):
    pl.semaphore_wait(pltpu.get_barrier_semaphore(), len(peers))


def dmas(n):
    return [pltpu.SemaphoreType.DMA((n,))] * 2


def comm(cid, **kw):
    return params(collective_id=cid, has_side_effects=True, **kw)


def other_core():
    return {'core': 1 - lax.axis_index('core')}


def along(axis, j, n):
    return {axis: lax.rem(lax.axis_index(axis) + j, n)}


def chip_peers(xs):
    here = lax.axis_index('x') * 2 + lax.axis_index('core')
    spots = [lax.rem(here + j, 2 * xs) for j in range(1, 2 * xs)]
    return [{'x': r // 2, 'core': lax.rem(r, 2)} for r in spots]


def pieces(x):
    return [x[:, g * LANES:(g + 1) * LANES] for g in range(x.shape[1] // LANES)]


def put_rows(ref, base, x):
    for g, piece in enumerate(pieces(x)):
        ref[base + g:base + g + 1, :] = piece


def norm_kernel(xs, h_ref, mask_ref, y_ref, inv_ref, count_ref, send, recv, ssem, rsem):
    peers = chip_peers(xs)
    hello(peers)
    send[...] = jnp.zeros(send.shape, F32)
    put_rows(send, 0, mask_ref[...])
    for r0 in range(0, h_ref.shape[0], LANES):
        rs = slice(r0, r0 + LANES)
        h = h_ref[rs, :].astype(F32)
        inv = lax.rsqrt(jnp.mean(h * h, axis=1, keepdims=True) + EPS_NORM)
        inv_ref[rs, :] = inv
        y_ref[rs, :] = h * inv
    meet(peers)
    links = Links(ssem, rsem)
    copies = [links.copy(send, recv.at[k], to) for k, to in enumerate(peers)]
    start(copies)
    wait(copies)
    total = send[...] + jnp.sum(recv[...], axis=0)
    count_ref[...] = jnp.broadcast_to(jnp.sum(total, keepdims=True), count_ref.shape)


def norm(hidden, mask, xs):
    tok, dim = hidden.shape
    n = 2 * xs - 1
    return pl.pallas_call(
        functools.partial(norm_kernel, xs),
        out_shape=(shape(tok, dim), shape(tok, 1), line(LANES)),
        in_specs=[VMEM] * 2,
        out_specs=(VMEM,) * 3,
        scratch_shapes=[pltpu.VMEM((SUB, LANES), F32), pltpu.VMEM((n, SUB, LANES), F32), *dmas(n)],
        compiler_params=comm(4),
        cost_estimate=cost(1e9, tok * dim * 6),
        name='norm',
    )(hidden, mask)


def sort_kernel(vocab, whole, ids_ref, pt_ref, mask_ref, y_hbm, out_ref, ypart_hbm, lpart_hbm, ssem, rsem):
    links = Links(ssem, rsem)
    to = other_core()
    y_copy, l_copy = links.copy(y_hbm, ypart_hbm, to), links.copy(out_ref, lpart_hbm, to)
    hello([to])
    meet([to])
    y_copy.start()
    n = ids_ref.shape[1]
    sub = iota(SUB, LANES)
    nv = n // SUB
    base = lax.axis_index('tp') * vocab
    for g in range(ids_ref.shape[0] // LANES):
        cols = slice(g * LANES, (g + 1) * LANES)
        order = ids_ref[cols, :] - base
        key = (jnp.where(order < 0, order + whole, order) + 1).astype(F32).T
        prob = pt_ref[cols, :].T
        k = [key[sub8(a), :] for a in range(nv)]
        p = [prob[sub8(a), :] for a in range(nv)]
        size = 2
        while size <= n:
            j = size // 2
            while j:
                if j >= SUB:
                    for a in range(nv):
                        if (SUB * a) & j:
                            continue
                        b = a + j // SUB
                        up = ((SUB * a) & size) == 0
                        swap = k[a] > k[b] if up else k[a] < k[b]
                        lo, hi = jnp.minimum(k[a], k[b]), jnp.maximum(k[a], k[b])
                        k[a], k[b] = (lo, hi) if up else (hi, lo)
                        p[a], p[b] = jnp.where(swap, p[b], p[a]), jnp.where(swap, p[a], p[b])
                else:
                    low = (sub & j) == 0
                    for a in range(nv):
                        if size >= SUB:
                            want_min = low if ((SUB * a) & size) == 0 else (sub & j) != 0
                        else:
                            want_min = low == ((sub & size) == 0)
                        ka = jnp.where(low, pltpu.roll(k[a], SUB - j, 0), pltpu.roll(k[a], j, 0))
                        pa = jnp.where(low, pltpu.roll(p[a], SUB - j, 0), pltpu.roll(p[a], j, 0))
                        new = jnp.where(want_min, jnp.minimum(k[a], ka), jnp.maximum(k[a], ka))
                        p[a] = jnp.where(new == ka, pa, p[a])
                        k[a] = new
                j //= 2
            size *= 2
        sign = jnp.where(mask_ref[:, cols] > 0, 1.0, -1.0)
        for a in range(nv):
            out_ref[sub8(a), cols] = k[a] * sign
            out_ref[sub8(nv + a), cols] = p[a]
    y_copy.wait()
    l_copy.start()
    l_copy.wait()


def sort_lists(ids, prob, mask, y, vocab, whole):
    tokens, top = ids.shape
    lists = shape(2 * top, tokens)
    return pl.pallas_call(
        functools.partial(sort_kernel, vocab, whole),
        out_shape=(lists, shape(*y.shape), lists),
        in_specs=[VMEM] * 3 + [ANY],
        out_specs=(VMEM, ANY, ANY),
        scratch_shapes=dmas(2),
        compiler_params=comm(5),
        cost_estimate=cost(LARGE, tokens * top * 16),
        name='sort_lists',
    )(ids, prob, mask, y)


def roll_all(x, op):
    for sh in (4, 2, 1):
        x = op(x, pltpu.roll(x, sh, 0))
    return x


def local_order(block, core, half):
    return jnp.abs(block).astype(I32) - 1 - core * half


def expand_kernel(vocab, half, plan, lane_block, *refs):
    lists, (w_ref, tabr_ref, tabp_ref, cnt_ref, src, loc_s, pw_s, sem) = refs[:-8], refs[-8:]
    g = step_id()
    groups = (last_step() + 1)
    core = lax.axis_index('core')
    rows = core_rows(vocab, half)
    top = src.shape[1] // 2
    nq = top // SUB
    nblk = half // LANES
    sub = iota(SUB, LANES)
    blank = jnp.zeros((SUB, LANES), I32)

    def fetch(k):
        which = plan(k, core)
        for a, ref in enumerate(lists):
            @pl.when(which == a)
            def _():
                pltpu.make_async_copy(ref.at[:, at(lane_block(k) * LANES, LANES)], src.at[k], sem.at[k]).start()

    @pl.when(g == 0)
    def _():
        cnt_ref[...] = jnp.zeros(cnt_ref.shape, I32)
        for k in range(src.shape[0]):
            fetch(k)

    pltpu.make_async_copy(lists[0].at[:, 0:LANES], src.at[g], sem.at[g]).wait()
    w = w_ref[...]
    over = blank
    used = blank
    first = jnp.full((SUB, LANES), nq, I32)
    prev = None
    for q in range(nq):
        order = local_order(src[g, sub8(q), :], core, half)
        ok = (order >= 0) & (order < rows)
        loc = jnp.where(ok, order, -1)
        loc_s[sub8(q), :] = loc
        pw_s[sub8(q), :] = src[g, sub8(nq + q), :] * w
        used = jnp.where(ok, q + 1, used)
        first = jnp.minimum(first, jnp.where(ok, q, nq))
        blk = loc >> 7
        if prev is not None:
            over = jnp.where((blk == prev) & ok, 1, over)
        prev = blk
    over = roll_all(over, jnp.maximum)
    lo, hi = jnp.min(first), jnp.max(used)

    def body(bt, carry):
        b0 = bt * SUB

        def scan(q, acc):
            accc, accp = list(acc[0]), list(acc[1])
            here = at(q * SUB, SUB)
            loc = loc_s[here, :]
            blk = (loc >> 7) - b0
            code = (sub + SUB * q) * LANES + (loc & (LANES - 1))
            p = pw_s[here, :]
            for i in range(SUB):
                m = blk == i
                accc[i] = jnp.where(m, code, accc[i])
                accp[i] = jnp.where(m, p, accp[i])
            return tuple(accc), tuple(accp)

        empty = (((blank - 1),) * SUB, (jnp.zeros((SUB, LANES), F32),) * SUB)
        accc, accp = lax.fori_loop(lo, hi, scan, empty)
        most = blank
        for i in range(SUB):
            code, p = accc[i], accp[i]
            head = roll_all(jnp.where(code >= 0, code, top * LANES), jnp.minimum)
            start_ = (head >> 7) & (SUB - 1)
            for sh in (1, 2, 4):
                move = (start_ & sh) != 0
                code = jnp.where(move, pltpu.roll(code, SUB - sh, 0), code)
                p = jnp.where(move, pltpu.roll(p, SUB - sh, 0), p)
            full = roll_all(jnp.where(code >= 0, sub + 1, 0), jnp.maximum)
            most = jnp.where(sub == i, full, most)
            row = at((b0 + i) * SUB, SUB)
            tabr_ref[row, :] = jnp.where(code >= 0, code & (LANES - 1), -1)
            tabp_ref[row, :] = p
        most = jnp.where(over > 0, SLOTS + 1, most)
        tile = at(b0, SUB)
        cnt_ref[tile, :] = jnp.maximum(cnt_ref[tile, :], most)
        return carry

    lax.fori_loop(0, nblk // SUB, body, 0)

    @pl.when(g == groups - 1)
    def _():
        most = jnp.max(cnt_ref[...].astype(F32), axis=1, keepdims=True)
        cnt_ref[...] = jnp.broadcast_to(most, cnt_ref.shape).astype(I32)


def expand(lists, plan, lane_block, weight, vocab, half):
    top = lists[0].shape[0] // 2
    groups = weight.shape[1] // LANES
    nblk = half // LANES
    width = groups * LANES

    def spec(rows):
        return pl.BlockSpec((rows, LANES), lambda g: (0, g))

    tabr, tabp, cnt = pl.pallas_call(
        functools.partial(expand_kernel, vocab, half, plan, lane_block),
        out_shape=(shape(nblk * SLOTS, width, I32), shape(nblk * SLOTS, width), shape(nblk, LANES, I32)),
        grid=(groups,),
        in_specs=[ANY] * len(lists) + [spec(1)],
        out_specs=(spec(nblk * SLOTS), spec(nblk * SLOTS), fixed(nblk, LANES)),
        scratch_shapes=[pltpu.VMEM((groups, 2 * top, LANES), F32), pltpu.VMEM((top, LANES), I32),
                        pltpu.VMEM((top, LANES), F32), pltpu.SemaphoreType.DMA((groups,))],
        compiler_params=params(dimension_semantics=ORDERED),
        cost_estimate=cost(groups * SMALL, 4 * width * (2 * top + 2 * nblk * SLOTS)),
    )(*lists, weight)
    return (tabr, tabp), cnt


def put_tokens(y_ref, dest, scale_ref, ut_ref, u_ref):
    here = at(dest, y_ref.shape[0])
    cols = u_ref.shape[1] // 2
    ut_ref[:, here] = (y_ref[...] * scale_ref[...]).astype(BF16).T
    core = lax.axis_index('core')
    for k, c in enumerate((core, 1 - core)):
        mine = at((2 * lax.axis_index('x') + c) * cols, cols)
        u_ref[here, k * cols:(k + 1) * cols] = (y_ref[:, mine] * scale_ref[:, mine]).astype(BF16)


def tiles(vocab, half, e_ref, ut_ref, z_ref, m_ref, s_ref):
    vb = e_ref.shape[0]
    i = step_id()
    left = core_rows(vocab, half) - i * vb

    @pl.when(i == 0)
    def _():
        m_ref[...] = jnp.full(m_ref.shape, NEG, F32)
        s_ref[...] = jnp.zeros(s_ref.shape, F32)

    for r0 in range(0, vb, TILE):
        rs = slice(r0, r0 + TILE)
        keep = iota(TILE, WIDE) < left - r0
        for c0 in range(0, ut_ref.shape[1], WIDE):
            cs = slice(c0, c0 + WIDE)
            z = jnp.dot(e_ref[rs, :], ut_ref[:, cs], preferred_element_type=F32)
            z = jnp.where(keep, z, NEG)
            z_ref[rs, cs] = z
            z3 = z.reshape(TILE // SUB, SUB, WIDE)
            old = m_ref[:, cs]
            new = jnp.maximum(old, jnp.max(z3, axis=0))
            m_ref[:, cs] = new
            s_ref[:, cs] = s_ref[:, cs] * jnp.exp(old - new) + jnp.sum(jnp.exp(z3 - new[None]), axis=0)


def own_kernel(vocab, half, y_ref, ypart_ref, scale_ref, e_ref, z_ref, m_ref, s_ref, u_ref, ut_ref):
    @pl.when(step_id() == 0)
    def _():
        tok = y_ref.shape[0]
        core = lax.axis_index('core')
        put_tokens(y_ref, core * tok, scale_ref, ut_ref, u_ref)
        put_tokens(ypart_ref, (1 - core) * tok, scale_ref, ut_ref, u_ref)

    tiles(vocab, half, e_ref, ut_ref, z_ref, m_ref, s_ref)


class Square:
    def __init__(self, n):
        t = lax.axis_index('tp')
        self.z, self.y, self.n = t // n, lax.rem(t, n), n
        self.zs = [lax.rem(self.z + j, n) for j in range(1, n)]
        self.ys = [lax.rem(self.y + j, n) for j in range(1, n)]
        self.along_z = [{'tp': z * n + self.y} for z in self.zs]
        self.along_y = [{'tp': self.z * n + y} for y in self.ys]
        self.peers = self.along_z + self.along_y


def x_peers(xs):
    return [along('x', 1, xs), along('x', xs - 1, xs)]


def gather_tokens(srcs, own, part, lsem, links):
    here = [pltpu.make_async_copy(src, own.at[k], lsem.at[k]) for k, src in enumerate(srcs)]
    there = [links.copy(src, part.at[k], other_core()) for k, src in enumerate(srcs)]
    return here, there


def place_tokens(here, there, own, part, scale_ref, ut_ref, u_ref):
    n = own.shape[1]
    core = lax.axis_index('core')
    wait(here)
    for k in range(own.shape[0]):
        put_tokens(own.at[k], (2 * k + core) * n, scale_ref, ut_ref, u_ref)
    wait(there)
    for k in range(own.shape[0]):
        put_tokens(part.at[k], (2 * k + 1 - core) * n, scale_ref, ut_ref, u_ref)


def near_kernel(xs, n, vocab, half, left, right, du, ysl_ref, scale_ref, e_ref,
                z_ref, m_ref, s_ref, u_ref, far0, far1, rest_ref, dw_ref,
                ut_ref, own, part, a1, b1, sa, sb, a2, b2, lsem, ssem, rsem):
    i = step_id()
    sq = Square(n)
    links = Links(ssem, rsem)
    cut = far0.shape[0]
    h = du.shape[3] // 2
    ahead, behind = x_peers(xs)
    here, there = gather_tokens((left, right), own, part, lsem, links)
    far = [links.copy(left.at[:cut, :], far0, ahead), links.copy(right.at[cut:2 * cut, :], far1, behind)]
    first, second = [], []
    for j, (z, y, to_z, to_y) in enumerate(zip(sq.zs, sq.ys, sq.along_z, sq.along_y)):
        k = j + 1
        first.append(links.copy(du.at[:, y, :, :h], a1.at[k], to_y))
        first.append(links.copy(du.at[z, :, :, h:2 * h], b1.at[k], to_z))
        second.append(links.copy(sa.at[z], a2.at[j], to_z))
        second.append(links.copy(sb.at[y], b2.at[j], to_y))
    mine = [pltpu.make_async_copy(du.at[:, sq.y, :, :h], a1.at[0], lsem.at[2]),
            pltpu.make_async_copy(du.at[sq.z, :, :, h:2 * h], b1.at[0], lsem.at[3])]
    peers = [other_core(), ahead, behind, *sq.peers]

    @pl.when(i == 0)
    def _():
        start(here)
        start(mine)
        hello(peers)
        meet(peers)
        start(there)
        start(first)
        start(far)
        place_tokens(here, there, own, part, scale_ref, ut_ref, u_ref)

    tiles(vocab, half, e_ref, ut_ref, z_ref, m_ref, s_ref)

    @pl.when(i == (last_step() + 1) - 3)
    def _():
        wait(mine)
        wait(first)
        sa[...] = jnp.sum(a1[...], axis=0)
        sb[...] = jnp.sum(b1[...], axis=0)

    @pl.when(i == (last_step() + 1) - 2)
    def _():
        start(second)

    @pl.when(i == last_step())
    def _():
        wait(second)
        parts = ((sa[sq.z] + jnp.sum(a2[...], axis=0), slice(h)), (sb[sq.y] + jnp.sum(b2[...], axis=0), slice(h, 2 * h)))
        dot = 0.0
        for du_sum, cs in parts:
            y = ysl_ref[:, cs]
            dot = dot + jnp.sum(du_sum * scale_ref[:, cs] * y, axis=1, keepdims=True)
            dw_ref[:, cs] = jnp.sum(du_sum * y, axis=0, keepdims=True)
        mean = dot / (2 * h)
        for du_sum, cs in parts:
            rest_ref[:, cs] = du_sum * scale_ref[:, cs] - ysl_ref[:, cs] * mean
        wait(far)


def far_kernel(xs, n, vocab, half, far0, far1, lists, rest_ref, scale_ref, e_ref,
               z_ref, m_ref, s_ref, u_ref, dh, l_left, p_left, l_right, p_right, l_far, p_far,
               ut_ref, own, part, lsem, ssem, rsem):
    i = step_id()
    sq = Square(n)
    links = Links(ssem, rsem)
    h = rest_ref.shape[1] // 2
    rows = lists.shape[0] // 2
    ahead, behind = x_peers(xs)
    core = other_core()
    here, there = gather_tokens((far0, far1), own, part, lsem, links)
    lists1 = [links.copy(lists, l_left, ahead), links.copy(lists, l_right, behind)]
    lists2 = [links.copy(l_left.at[:rows, :], l_far.at[:rows, :], ahead),
              links.copy(l_right.at[rows:2 * rows, :], l_far.at[rows:2 * rows, :], behind),
              links.copy(l_left, p_left, core), links.copy(l_right, p_right, core)]
    lists3 = [links.copy(l_far, p_far, core)]
    first, second = [], []
    a, b = slice(h), slice(h, 2 * h)
    z, y = sq.z, sq.y
    for to_z, to_y in zip(sq.along_z, sq.along_y):
        first.append(links.copy(rest_ref.at[:, a], dh.at[z, y, :, a], to_z))
        first.append(links.copy(rest_ref.at[:, b], dh.at[z, y, :, b], to_y))
        second.append(links.copy(dh.at[:, y, :, a], dh.at[:, y, :, a], to_y))
        second.append(links.copy(dh.at[z, :, :, b], dh.at[z, :, :, b], to_z))
    mine = [pltpu.make_async_copy(rest_ref, dh.at[z, y], lsem.at[2])]
    peers = [core, ahead, behind, *sq.peers]

    @pl.when(i == 0)
    def _():
        start(here)
        start(mine)
        hello(peers)
        meet(peers)
        start(there)
        start(first)
        start(lists1)
        place_tokens(here, there, own, part, scale_ref, ut_ref, u_ref)

    tiles(vocab, half, e_ref, ut_ref, z_ref, m_ref, s_ref)

    @pl.when(i == 2)
    def _():
        wait(mine)
        wait(first)
        start(second)

    @pl.when(i == last_step())
    def _():
        wait(lists1)
        start(lists2)
        wait(lists2)
        start(lists3)
        wait(second)
        wait(lists3)


def forward(kernel, ins, in_specs, scale, emb, half, vb, width, outs=(), scratch=(), cid=None):
    vocab, dim = emb.shape
    nb = half // vb
    ccols = dim // 4
    return pl.pallas_call(
        functools.partial(kernel, vocab, half),
        out_shape=[shape(half, width), shape(SUB, width), shape(SUB, width), shape(width, ccols, BF16)] + [o for o, _ in outs],
        grid=(nb,),
        in_specs=in_specs + [one_row(dim), pl.BlockSpec((vb, dim), lambda i: (lax.axis_index('core') * nb + i, 0))],
        out_specs=[by_row(vb, width), fixed(SUB, width), fixed(SUB, width), fixed(width, ccols)] + [o for _, o in outs],
        scratch_shapes=[pltpu.VMEM((dim, width), BF16), *scratch],
        compiler_params=(params if cid is None else functools.partial(comm, cid))(dimension_semantics=ORDERED),
        cost_estimate=cost(2.0 * half * width * dim, half * dim * 2 + half * width * 4 + width * dim * 4, half * width),
    )(*ins, scale, emb)


def tokens_scratch(n, dim):
    return [pltpu.VMEM((2, n, dim), F32)] * 2


def stats_kernel(tps, xs, order, own, *refs):
    nlist = 2 * len(order)
    lists, refs = refs[:nlist], refs[nlist:]
    nstat = 2 if own else 4
    stat, refs = refs[:nstat], refs[nstat:]
    count_ref, refs = refs[0], refs[1:]
    if own:
        c_ref, w_ref, loss_ref, send, recv, ssem, rsem = refs
    else:
        dw_ref, tz_ref, loss0_ref, c_ref, w_ref, loss_ref, dwsum_ref, send, recv, xsend, xrecv, tsend, trecv, ssem, rsem = refs
    core = lax.axis_index('core')
    me = lax.axis_index('tp') * 2 + core
    spots = [lax.rem(me + j, 2 * tps) for j in range(1, 2 * tps)]
    peers = [{'tp': r // 2, 'core': lax.rem(r, 2)} for r in spots]
    near = [] if own else chip_peers(xs)
    gr = send.shape[0] // 2
    hello(peers + near)

    base = 0
    send[...] = jnp.zeros(send.shape, F32)
    for m_ref, s_ref in zip(stat[::2], stat[1::2]):
        m = jnp.max(m_ref[...], axis=0, keepdims=True)
        s = jnp.sum(s_ref[...] * jnp.exp(m_ref[...] - m), axis=0, keepdims=True)
        put_rows(send, base, m)
        put_rows(send, gr + base, s)
        base += m.shape[1] // LANES
    masks = []
    for chip, cuts in enumerate(order):
        for lanes in cuts:
            a, b = (ref[0:1, lanes] for ref in lists[2 * chip:2 * chip + 2])
            masks += [jnp.where(core == 0, a, b), jnp.where(core == 0, b, a)]
    mask = (jnp.concatenate(masks, axis=1) > 0).astype(F32)
    w = mask / count_ref[:, 0:1]
    w_ref[...] = w

    links = Links(ssem, rsem)
    copies = [links.copy(send, recv.at[k], to) for k, to in enumerate(peers)]
    if not own:
        xsend[...] = jnp.zeros(xsend.shape, F32)
        put_rows(xsend, 0, dw_ref[...])
        tz = functools.reduce(jnp.add, pieces(jnp.sum(tz_ref[...], axis=0, keepdims=True)))
        last = xsend.shape[0] - SUB
        xsend[last:last + 1, :] = tz
        xcopies = [links.copy(xsend, xrecv.at[k], to) for k, to in enumerate(near)]
        tcopies = [links.copy(tsend, trecv.at[j - 1], along('tp', j, tps)) for j in range(1, tps)]
    meet(peers + near)
    start(copies)
    if not own:
        start(xcopies)
        wait(xcopies)
        tsend[...] = xsend[...] + jnp.sum(xrecv[...], axis=0)
    wait(copies)
    if not own:
        start(tcopies)
    mine, theirs = send[:gr, :], recv[:, :gr, :]
    best = jnp.maximum(mine, jnp.max(theirs, axis=0))
    acc = send[gr:, :] * jnp.exp(mine - best) + jnp.sum(recv[:, gr:, :] * jnp.exp(theirs - best[None]), axis=0)
    lse = best + jnp.log(acc)
    lse = jnp.concatenate([lse[g:g + 1, :] for g in range(mask.shape[1] // LANES)], axis=1)
    c_ref[...] = jnp.where(mask > 0, lse - jnp.log(w), BIG)
    loss = functools.reduce(jnp.add, pieces(w * lse))
    if own:
        loss_ref[...] = loss
    else:
        wait(tcopies)
        total = tsend[...] + jnp.sum(trecv[...], axis=0)
        dwsum_ref[...] = jnp.concatenate([total[g:g + 1, :] for g in range(last)], axis=1)
        loss_ref[...] = jnp.sum(loss + loss0_ref[...] - total[last:last + 1, :], axis=1, keepdims=True)


def stats(lists, order, stat, count, tps, xs, cid, adds=()):
    own = not adds
    width = sum(m.shape[1] for m in stat[::2])
    tok = lists[0].shape[1]
    gr = -(-width // (LANES * SUB)) * SUB
    n = 2 * tps - 1
    outs = [line(width), line(width), line(LANES if own else 1)]
    scratch = [pltpu.VMEM((2 * gr, LANES), F32), pltpu.VMEM((n, 2 * gr, LANES), F32)]
    if not own:
        outs.append(shape(*adds[0].shape))
        xr = adds[0].shape[1] // LANES + SUB
        near = 2 * xs - 1
        scratch += [pltpu.VMEM((xr, LANES), F32), pltpu.VMEM((near, xr, LANES), F32),
                    pltpu.VMEM((xr, LANES), F32), pltpu.VMEM((tps - 1, xr, LANES), F32)]
        n += near + tps - 1
    return pl.pallas_call(
        functools.partial(stats_kernel, tps, xs, order, own),
        out_shape=outs,
        grid=(1,),
        in_specs=[fixed(SUB, tok)] * len(lists) + [fixed(*a.shape) for a in (*stat, count, *adds)],
        out_specs=[fixed(*o.shape) for o in outs],
        scratch_shapes=scratch + dmas(n),
        compiler_params=comm(cid),
        cost_estimate=cost(2e9, 1 << 16),
    )(*lists, *stat, count, *adds)


def fill_teacher(cnt_ref, first, nrb, tabr_ref, tabp_ref, w_ref, lists, plan, lane_block, half, tm, src, sem):
    width = tm.shape[1]
    core = lax.axis_index('core')
    rows = iota(LANES, LANES)
    zero = jnp.zeros((LANES, LANES), F32)
    top = src.shape[0] // 2

    def pick(row, val, t):
        for s in range(SUB):
            t = jnp.where(rows == row[s:s + 1, :], val[s:s + 1, :], t)
        return t

    for rb in range(nrb):
        n = cnt_ref[first + rb, 0]
        rs = slice(rb * LANES, (rb + 1) * LANES)

        def tile(g, carry):
            lanes = at(g * LANES, LANES)

            @pl.when(n <= SLOTS)
            def _():
                tm[rs, lanes] = pick(tabr_ref[sub8(rb), lanes], tabp_ref[sub8(rb), lanes], zero)

            @pl.when(n > SLOTS)
            def _():
                which = plan(g, core)
                for a, ref in enumerate(lists):
                    @pl.when(which == a)
                    def _():
                        copy = pltpu.make_async_copy(ref.at[:, at(lane_block(g) * LANES, LANES)], src, sem.at[0])
                        copy.start()
                        copy.wait()
                w = w_ref[:, lanes]

                def entries(k, t):
                    order = local_order(src[at(k * SUB, SUB), :], core, half) - (first + rb) * LANES
                    return pick(order, src[at(top + k * SUB, SUB), :] * w, t)

                tm[rs, lanes] = lax.fori_loop(0, top // SUB, entries, zero)

            return carry

        lax.fori_loop(0, width // LANES, tile, 0)


def g_tile(z_ref, z0, c_ref, cs, rb, tabr_ref, tabp_ref, tm, put):
    c = c_ref[:, cs]
    step = 2 * SUB
    rows = iota(step, TILE)
    slots = range(SUB * rb, SUB * rb + FAST)
    ids = [jnp.broadcast_to(tabr_ref[s:s + 1, cs], (step, TILE)) for s in slots]
    vals = [tabp_ref[s:s + 1, cs] for s in slots]
    for r0 in range(0, LANES, step):
        rs = slice(rb * LANES + r0, rb * LANES + r0 + step)
        z = z_ref[rs, z0:z0 + TILE]
        if tm is None:
            t = jnp.zeros((step, TILE), F32)
            for row, val in zip(ids, vals):
                t = jnp.where(rows + r0 == row, val, t)
        else:
            t = tm[rs, cs]
        put(rs, (jnp.exp(z - c) - t).astype(BF16), t, z)


def most_slots(cnt_ref, first, nrb):
    n = cnt_ref[first, 0]
    for rb in range(1, nrb):
        n = jnp.maximum(n, cnt_ref[first + rb, 0])
    return n


def fill_scratch(vb, width, lists):
    return [pltpu.VMEM((vb, width), F32), pltpu.VMEM((lists[0].shape[0], LANES), F32), pltpu.SemaphoreType.DMA((1,))]


def g_kernel(half, plan, lane_block, cnt_ref, z_ref, c_ref, tabr_ref, tabp_ref, w_ref, *refs):
    lists, (g_ref, gt_ref, tz_ref, tm, src, sem) = refs[:-6], refs[-6:]
    i = step_id()
    vb, width = z_ref.shape
    nrb = vb // LANES

    @pl.when(i == 0)
    def _():
        tz_ref[...] = jnp.zeros(tz_ref.shape, F32)

    slots = most_slots(cnt_ref, i * nrb, nrb)

    def make(full):
        for c0 in range(0, width, TILE):
            cs = slice(c0, c0 + TILE)
            acc = [jnp.zeros((SUB, TILE), F32)]

            def put(rs, g, t, z):
                g_ref[rs, cs] = g
                tz = t * z
                acc[0] = acc[0] + tz[:SUB] + tz[SUB:]

            for rb in range(nrb):
                g_tile(z_ref, c0, c_ref, cs, rb, tabr_ref, tabp_ref, full, put)
                rs = slice(rb * LANES, (rb + 1) * LANES)
                gt_ref[cs, rs] = g_ref[rs, cs].T
            tz_ref[:, cs] += acc[0]

    @pl.when(slots <= FAST)
    def _():
        make(None)

    @pl.when(slots > FAST)
    def _():
        fill_teacher(cnt_ref, i * nrb, nrb, tabr_ref, tabp_ref, w_ref, lists, plan, lane_block, half, tm, src, sem)
        make(tm)


def g_own(cnt, z, c, tables, w, lists, plan, lane_block):
    half, width = z.shape
    vb = WIDE
    trows = vb // LANES * SLOTS

    def row(i, n):
        return (i, 0)

    return pl.pallas_call(
        functools.partial(g_kernel, half, plan, lane_block),
        out_shape=(shape(half, width, BF16), shape(width, half, BF16), shape(SUB, width)),
        grid_spec=pltpu.PrefetchScalarGridSpec(
            num_scalar_prefetch=1,
            grid=(half // vb,),
            in_specs=[pl.BlockSpec((vb, width), row), one_row(width), pl.BlockSpec((trows, width), row),
                      pl.BlockSpec((trows, width), row), one_row(width)] + [ANY] * len(lists),
            out_specs=(pl.BlockSpec((vb, width), row), pl.BlockSpec((width, vb), lambda i, n: (0, i)), fixed(SUB, width)),
            scratch_shapes=fill_scratch(vb, width, lists),
        ),
        compiler_params=params(dimension_semantics=ORDERED),
        cost_estimate=cost(LARGE, half * width * 8, half * width),
        name='g_own',
    )(cnt, z, c, *tables, w, *lists)


def du_kernel(vocab, half, gt_ref, e_ref, out_ref, mine, send, recv, ssem, rsem):
    i = step_id()
    core = lax.axis_index('core')
    rows = core_rows(vocab, half)
    tok = out_ref.shape[0]
    tiles = (last_step() + 1) - 2
    cut = (vocab - half) // TILE * TILE

    @pl.when(i == 0)
    def _():
        hello([other_core()])
        meet([other_core()])

    def copy(k):
        return pltpu.make_async_remote_copy(
            src_ref=send.at[k], dst_ref=recv.at[k], send_sem=ssem.at[k], recv_sem=rsem.at[k],
            device_id=other_core(), device_id_type=MESH)

    @pl.when((i >= 1) & (i <= tiles))
    def _():
        copy(i - 1).start()

    @pl.when(i < tiles)
    def _():
        tail = e_ref[cut:, :]
        tail = jnp.where(iota(*tail.shape) < rows - cut, tail, jnp.zeros((), BF16))

        def part(which):
            g = gt_ref[at(which * tok, tok), :]
            return (jnp.dot(g[:, :cut], e_ref[:cut, :], preferred_element_type=F32)
                    + jnp.dot(g[:, cut:], tail, preferred_element_type=F32))

        send[i] = part(1 - core)
        mine[i] = part(core)

    @pl.when(i >= 2)
    def _():
        copy(i - 2).wait()
        out_ref[...] = mine[i - 2] + recv[i - 2]


def du_call(gt, emb, half):
    vocab, dim = emb.shape
    tok = gt.shape[0] // 2
    tiles = dim // WIDE
    buf = pltpu.VMEM((tiles, tok, WIDE), F32)
    dma = pltpu.SemaphoreType.DMA((tiles,))
    return pl.pallas_call(
        functools.partial(du_kernel, vocab, half),
        out_shape=shape(tok, dim),
        grid=(tiles + 2,),
        in_specs=[fixed(*gt.shape),
                  pl.BlockSpec((half, WIDE), lambda i: (lax.axis_index('core'), jnp.minimum(i, tiles - 1)))],
        out_specs=pl.BlockSpec((tok, WIDE), lambda i: (0, jnp.maximum(i - 2, 0))),
        scratch_shapes=[buf, buf, buf, dma, dma],
        compiler_params=comm(2, dimension_semantics=ORDERED),
        cost_estimate=cost(4.0 * half * tok * dim, half * dim * 2),
        name='grad_u',
    )(gt, emb)


def de_kernel(half, b0, nu, plan, lane_block, cnt_ref, *refs):
    u_refs, refs = refs[:nu], refs[nu:]
    zn_ref, zf_ref, gown_ref, c_ref, tabr_ref, tabp_ref, w_ref = refs[:7]
    lists = refs[7:13]
    out_ref, part_ref, u_ref, g_ref, tm, src, sem = refs[-7:]
    i = step_id()
    vb, mine = gown_ref.shape
    cols = out_ref.shape[1]
    nrb = vb // LANES
    first = (b0 + i) * nrb

    @pl.when(i == 0)
    def _():
        base = 0
        for ref in u_refs:
            u_ref[base:base + ref.shape[0], :] = ref[...]
            base += ref.shape[0]

    def make(full):
        acc = jnp.dot(gown_ref[...], u_ref[:mine, :], preferred_element_type=F32)
        c0 = 0
        for z_ref in (zn_ref, zf_ref):
            for z0 in range(0, z_ref.shape[1], TILE):
                cs = slice(c0, c0 + TILE)

                def put(rs, g, t, z):
                    g_ref[rs, cs] = g

                for rb in range(nrb):
                    g_tile(z_ref, z0, c_ref, cs, rb, tabr_ref, tabp_ref, full, put)
                acc = acc + jnp.dot(g_ref[:, cs], u_ref[mine + c0:mine + c0 + TILE, :], preferred_element_type=F32)
                c0 += TILE
        out_ref[...] = acc[:, :cols]
        part_ref[...] = acc[:, cols:]

    slots = most_slots(cnt_ref, first, nrb)

    @pl.when(slots <= FAST)
    def _():
        make(None)

    @pl.when(slots > FAST)
    def _():
        fill_teacher(cnt_ref, first, nrb, tabr_ref, tabp_ref, w_ref, lists, plan, lane_block, half, tm, src, sem)
        make(tm)


def de_call(cnt, us, zn, zf, gown, c, tables, w, lists, plan, lane_block, vocab, b0, nb, prev):
    half, mine = gown.shape
    ccols = us[0].shape[1]
    cols = ccols // 2
    tot = half // TILE
    width = zn.shape[1] + zf.shape[1]
    trows = TILE // LANES * SLOTS

    def rows(cols_, height=TILE):
        return pl.BlockSpec((height, cols_), lambda i, n: (b0 + i, 0))

    in_specs = [fixed(*u.shape) for u in us]
    in_specs += [rows(zn.shape[1]), rows(zf.shape[1]), rows(mine), one_row(width), rows(width, trows), rows(width, trows),
                 one_row(width)] + [ANY] * len(lists)
    args = [*us, zn, zf, gown, c, *tables, w, *lists]
    aliases = {}
    if prev is not None:
        aliases = {1 + len(args): 0}
        args.append(prev)
        in_specs.append(ANY)
    return pl.pallas_call(
        functools.partial(de_kernel, half, b0, len(us), plan, lane_block),
        out_shape=(shape(vocab, cols), shape(nb * TILE, cols)),
        grid_spec=pltpu.PrefetchScalarGridSpec(
            num_scalar_prefetch=1,
            grid=(nb,),
            in_specs=in_specs,
            out_specs=(
                pl.BlockSpec((TILE, cols), lambda i, n: (lax.axis_index('core') * tot + b0 + i, 0)),
                pl.BlockSpec((TILE, cols), lambda i, n: (i, 0)),
            ),
            scratch_shapes=[pltpu.VMEM((width + mine, ccols), BF16), pltpu.VMEM((TILE, width), BF16),
                            *fill_scratch(TILE, width, lists)],
        ),
        input_output_aliases=aliases,
        compiler_params=params(dimension_semantics=ORDERED),
        cost_estimate=cost(3.0 * nb * TILE * (width + mine) * ccols, nb * TILE * (width * 4 + mine * 2 + ccols * 4),
                           nb * TILE * width),
    )(cnt, *args)


def place_kernel(half_blocks, a_ref, b_ref, prev_ref, out_ref):
    i = step_id()
    for k, ref in enumerate((a_ref, b_ref)):
        @pl.when(i // half_blocks == k)
        def _():
            out_ref[...] = ref[...]


def place(recvs, out, half):
    cols = out.shape[1]
    step = 2 * WIDE
    n = recvs[0].shape[0] // step
    return pl.pallas_call(
        functools.partial(place_kernel, n),
        out_shape=shape(*out.shape),
        grid=(2 * n,),
        in_specs=[pl.BlockSpec((step, cols), lambda i: (jnp.minimum(i, n - 1), 0)),
                  pl.BlockSpec((step, cols), lambda i: (jnp.maximum(i - n, 0), 0)), ANY],
        out_specs=pl.BlockSpec((step, cols), lambda i: ((1 - lax.axis_index('core')) * (half // step) + i, 0)),
        input_output_aliases={2: 0},
        compiler_params=params(),
        cost_estimate=cost(SMALL, out.size * 4),
        name='place',
    )(*recvs, out)


def dh_kernel(d_ref, inv_ref, out_ref):
    out_ref[...] = (inv_ref[...] * d_ref[...]).astype(BF16)


def dh_call(d, inv):
    tok, dim = d.shape
    step = tok // 4
    return pl.pallas_call(
        dh_kernel,
        out_shape=shape(tok, dim, BF16),
        grid=(tok // step,),
        in_specs=[by_row(step, dim), by_row(step, 1)],
        out_specs=by_row(step, dim),
        compiler_params=params(),
        cost_estimate=cost(SMALL, tok * dim * 6),
        name='grad_h',
    )(d, inv)


def solution(mesh):
    tps = mesh.shape['tp']
    xs = mesh.shape['dp'] // 2
    n = round(tps ** 0.5)
    grid = Mesh(np.asarray(mesh.devices).reshape(tps, xs, 2), ('tp', 'x', 'core'))

    def shift(x, axis, by):
        size = grid.shape[axis]
        return lax.ppermute(x, axis, [(i, (i + by) % size) for i in range(size)])

    def local_head(hidden, embedding, norm_weight, teach_ids, teach_prob, tok_mask):
        vocab, dim = embedding.shape
        tok = hidden.shape[0]
        chip = 2 * tok
        half = -(-vocab // (2 * WIDE)) * WIDE
        part = tok // tps
        cut = tok // 2
        tg = tok // LANES
        scale = (1.0 + norm_weight).reshape(row_of(norm_weight))
        mask = tok_mask.reshape(row_of(tok_mask))

        normed, inv_rms, count = norm(hidden, mask, xs)
        left = shift(normed, 'x', 1)
        right = shift(normed, 'x', -1)
        lists, y_part, l_part = sort_lists(teach_ids, teach_prob, mask, normed, vocab, vocab * tps)

        z0, m0, s0, u0 = forward(own_kernel, [normed, y_part], [fixed(tok, dim)] * 2, scale, embedding, half, 2 * WIDE,
                                 chip)
        full = slice(tok)
        lo, hi = slice(cut), slice(cut, tok)
        c0, w0, loss0 = stats([lists, l_part], ((full,),), (m0, s0), count, tps, xs, 0)
        own_plan = (lambda g, c: lax.rem(g // tg + c, 2)), (lambda g: lax.rem(g, tg))
        tab0, cnt0 = expand([lists, l_part], *own_plan, w0, vocab, half)
        g0, gt0, tz = g_own(cnt0, z0, c0, tab0, w0, [lists, l_part], *own_plan)
        du = du_call(gt0, embedding, half)

        my_normed = lax.dynamic_slice(normed, (lax.axis_index('tp') * part, 0), (part, dim))
        square = pltpu.VMEM((n, n, part, dim // 2), F32)
        strip = pltpu.VMEM((n, part, dim // 2), F32)
        short = pltpu.VMEM((n - 1, part, dim // 2), F32)
        dma = pltpu.SemaphoreType.DMA
        z1, m1, s1, u1, far0, far1, d_rest, dw = forward(
            functools.partial(near_kernel, xs, n), [left, right, du.reshape(n, n, part, dim), my_normed],
            [ANY] * 3 + [fixed(part, dim)], scale, embedding, half, WIDE, 2 * chip,
            outs=[(shape(cut, dim), ANY)] * 2 + [(shape(part, dim), fixed(part, dim)), (line(dim), one_row(dim))],
            scratch=[*tokens_scratch(tok, dim), square, square, strip, strip, short, short, dma((4,)),
                     *dmas(4 + 4 * (n - 1))], cid=3)
        one = (shape(*lists.shape), ANY)
        z2, m2, s2, u2, dh, *l_rest = forward(
            functools.partial(far_kernel, xs, n), [far0, far1, lists, d_rest], [ANY] * 3 + [fixed(part, dim)],
            scale, embedding, half, WIDE, chip,
            outs=[(jax.ShapeDtypeStruct((n, n, part, dim), F32), ANY)] + [one] * 6,
            scratch=[*tokens_scratch(cut, dim), dma((3,)), *dmas(9 + 4 * (n - 1))], cid=6)
        c1, w1, loss, dw_sum = stats(l_rest, ((full,), (full,), (lo, hi)), (m1, s1, m2, s2), count, tps, xs, 1,
                                     (dw, tz, loss0))

        def plan(g, c):
            far = g // (2 * tg) == 2
            swap = jnp.where(far, lax.rem(g, 2), lax.rem(g // tg, 2))
            return g // (2 * tg) * 2 + lax.rem(swap + c, 2)

        def lane_block(g):
            return jnp.where(g // (2 * tg) == 2, lax.rem(g // 2, tg), lax.rem(g, tg))

        rest_plan = plan, lane_block
        tab1, cnt1 = expand(l_rest, *rest_plan, w1, vocab, half)

        nb = half // TILE
        n0 = nb // 2

        def grad_e(b0, count_, prev):
            return de_call(cnt1, [u0, u1, u2], z1, z2, g0, c1, tab1, w1, l_rest, *rest_plan, vocab, b0, count_, prev)

        out, send0 = grad_e(0, n0, None)
        recv0 = shift(send0, 'core', 1)
        out, send1 = grad_e(n0, nb - n0, out)
        recv1 = shift(send1, 'core', 1)
        grad_hidden = dh_call(dh.reshape(tok, dim), inv_rms)
        out = place([recv0, recv1], out, half)
        return loss.reshape(()), grad_hidden, out, dw_sum.reshape(dim)

    tokens = ('x', 'core')
    return jax.shard_map(
        local_head,
        mesh=grid,
        in_specs=(P(tokens, None), P('tp', None), P(None), P(tokens, None), P(tokens, None), P(tokens)),
        out_specs=(P(), P(tokens, None), P('tp', tokens), P(None)),
        check_vma=False,
    )
```

```python
import functools

import jax
import jax.numpy as jnp
import numpy as np
from jax import lax
from jax.experimental import pallas as pl
from jax.experimental.pallas import tpu as pltpu
from jax.sharding import Mesh
from jax.sharding import PartitionSpec as P


EPS_NORM = 1e-6
BIG = 1e30
NEG = -BIG
SMALL, LARGE = 1e8, 4e9
F32, BF16, I32 = jnp.float32, jnp.bfloat16, jnp.int32
LANES, SUB = 128, 8
ORDERED = ('arbitrary',)
SLOTS = 8
FAST = 2
TILE = 256
WIDE = 512
VMEM_LIMIT = 60 * 1024 * 1024
MESH = pl.DeviceIdType.MESH
VMEM = pl.BlockSpec(memory_space=pltpu.VMEM)
ANY = pl.BlockSpec(memory_space=pltpu.HBM)


def params(**kw):
    return pltpu.CompilerParams(vmem_limit_bytes=VMEM_LIMIT, **kw)


def cost(flops, nbytes, trans=0):
    return pl.CostEstimate(flops=int(flops), bytes_accessed=int(nbytes), transcendentals=int(trans))


def shape(rows, cols, dtype=F32):
    return jax.ShapeDtypeStruct((rows, cols), dtype)


def fixed(rows, cols):
    return pl.BlockSpec((rows, cols), lambda *a: (0, 0))


def one_row(cols):
    return fixed(1, cols)


def by_row(rows, cols):
    return pl.BlockSpec((rows, cols), lambda i: (i, 0))


def sub8(a):
    return slice(SUB * a, SUB * a + SUB)


def iota(rows, cols, axis=0):
    return lax.broadcasted_iota(I32, (rows, cols), axis)


def at(start, size):
    return pl.ds(pl.multiple_of(start, size), size)


def step_id():
    return pl.program_id(0)


def last_step():
    return pl.num_programs(0) - 1


def row_of(x):
    return (1, x.size)


def line(cols):
    return shape(1, cols)


def core_rows(vocab, half):
    return jnp.where(lax.axis_index('core') == 0, half, vocab - half)


class Links:
    def __init__(self, ssem, rsem):
        self.ssem, self.rsem, self.used = ssem, rsem, 0

    def copy(self, src, dst, to):
        k = self.used
        self.used += 1
        return pltpu.make_async_remote_copy(
            src_ref=src, dst_ref=dst, send_sem=self.ssem.at[k], recv_sem=self.rsem.at[k], device_id=to, device_id_type=MESH)


def start(copies):
    for c in copies:
        c.start()


def wait(copies):
    for c in copies:
        c.wait()


def hello(peers):
    for to in peers:
        pl.semaphore_signal(pltpu.get_barrier_semaphore(), inc=1, device_id=to, device_id_type=MESH)


def meet(peers):
    pl.semaphore_wait(pltpu.get_barrier_semaphore(), len(peers))


def dmas(n):
    return [pltpu.SemaphoreType.DMA((n,))] * 2


def comm(cid, **kw):
    return params(collective_id=cid, has_side_effects=True, **kw)


def other_core():
    return {'core': 1 - lax.axis_index('core')}


def along(axis, j, n):
    return {axis: lax.rem(lax.axis_index(axis) + j, n)}


def chip_peers(xs):
    here = lax.axis_index('x') * 2 + lax.axis_index('core')
    spots = [lax.rem(here + j, 2 * xs) for j in range(1, 2 * xs)]
    return [{'x': r // 2, 'core': lax.rem(r, 2)} for r in spots]


def pieces(x):
    return [x[:, g * LANES:(g + 1) * LANES] for g in range(x.shape[1] // LANES)]


def to_row(x, rows):
    return jnp.concatenate([x[g:g + 1, :] for g in range(rows)], axis=1)


def total(ref):
    return jnp.sum(ref[...], axis=0)


def zeros(ref, dtype=F32):
    return jnp.zeros(ref.shape, dtype)


def put_rows(ref, base, x):
    for g, piece in enumerate(pieces(x)):
        ref[base + g:base + g + 1, :] = piece


def norm_kernel(xs, h_ref, mask_ref, y_ref, inv_ref, count_ref, send, recv, ssem, rsem):
    peers = chip_peers(xs)
    hello(peers)
    send[...] = zeros(send)
    put_rows(send, 0, mask_ref[...])
    links = Links(ssem, rsem)
    copies = [links.copy(send, recv.at[k], to) for k, to in enumerate(peers)]
    half = h_ref.shape[0] // 2
    for r0 in (0, half):
        rs = slice(r0, r0 + half)
        h = h_ref[rs, :].astype(F32)
        inv = lax.rsqrt(jnp.mean(h * h, axis=1, keepdims=True) + EPS_NORM)
        inv_ref[rs, :] = inv
        y_ref[rs, :] = h * inv
        if r0 == 0:
            meet(peers)
            start(copies)
    wait(copies)
    both = send[...] + total(recv)
    count_ref[...] = jnp.broadcast_to(jnp.sum(both, keepdims=True), count_ref.shape)


def norm(hidden, mask, xs):
    tok, dim = hidden.shape
    n = 2 * xs - 1
    return pl.pallas_call(
        functools.partial(norm_kernel, xs),
        out_shape=(shape(tok, dim), shape(tok, 1), line(LANES)),
        in_specs=[VMEM] * 2,
        out_specs=(VMEM,) * 3,
        scratch_shapes=[pltpu.VMEM((SUB, LANES), F32), pltpu.VMEM((n, SUB, LANES), F32), *dmas(n)],
        compiler_params=comm(4),
        cost_estimate=cost(1e9, tok * dim * 6),
        name='norm',
    )(hidden, mask)


def sort_kernel(vocab, whole, ids_ref, pt_ref, mask_ref, y_hbm, out_ref, ypart_hbm, ssem, rsem):
    links = Links(ssem, rsem)
    to = other_core()
    y_copy = links.copy(y_hbm, ypart_hbm, to)
    hello([to])
    meet([to])
    y_copy.start()
    n = ids_ref.shape[1]
    sub = iota(SUB, LANES)
    nv = n // SUB
    base = lax.axis_index('tp') * vocab
    for g in range(ids_ref.shape[0] // LANES):
        cols = slice(g * LANES, (g + 1) * LANES)
        order = ids_ref[cols, :] - base
        key = (jnp.where(order < 0, order + whole, order) + 1).astype(F32).T
        prob = pt_ref[cols, :].T
        k = [key[sub8(a), :] for a in range(nv)]
        p = [prob[sub8(a), :] for a in range(nv)]
        size = 2
        while size <= n:
            j = size // 2
            while j:
                if j >= SUB:
                    for a in range(nv):
                        if (SUB * a) & j:
                            continue
                        b = a + j // SUB
                        up = ((SUB * a) & size) == 0
                        swap = k[a] > k[b] if up else k[a] < k[b]
                        lo, hi = jnp.minimum(k[a], k[b]), jnp.maximum(k[a], k[b])
                        k[a], k[b] = (lo, hi) if up else (hi, lo)
                        p[a], p[b] = jnp.where(swap, p[b], p[a]), jnp.where(swap, p[a], p[b])
                else:
                    low = (sub & j) == 0
                    for a in range(nv):
                        if size >= SUB:
                            want_min = low if ((SUB * a) & size) == 0 else (sub & j) != 0
                        else:
                            want_min = low == ((sub & size) == 0)
                        ka = jnp.where(low, pltpu.roll(k[a], SUB - j, 0), pltpu.roll(k[a], j, 0))
                        pa = jnp.where(low, pltpu.roll(p[a], SUB - j, 0), pltpu.roll(p[a], j, 0))
                        new = jnp.where(want_min, jnp.minimum(k[a], ka), jnp.maximum(k[a], ka))
                        p[a] = jnp.where(new == ka, pa, p[a])
                        k[a] = new
                j //= 2
            size *= 2
        sign = jnp.where(mask_ref[:, cols] > 0, 1.0, -1.0)
        for a in range(nv):
            out_ref[sub8(a), cols] = k[a] * sign
            out_ref[sub8(nv + a), cols] = p[a]
    y_copy.wait()


def sort_lists(ids, prob, mask, y, vocab, whole):
    tokens, top = ids.shape
    lists = shape(2 * top, tokens)
    return pl.pallas_call(
        functools.partial(sort_kernel, vocab, whole),
        out_shape=(lists, shape(*y.shape)),
        in_specs=[VMEM] * 3 + [ANY],
        out_specs=(VMEM, ANY),
        scratch_shapes=dmas(1),
        compiler_params=comm(7),
        cost_estimate=cost(LARGE, tokens * top * 16),
        name='sort_lists',
    )(ids, prob, mask, y)


def roll_all(x, op):
    for sh in (4, 2, 1):
        x = op(x, pltpu.roll(x, sh, 0))
    return x


def local_order(block, core, half):
    return jnp.abs(block).astype(I32) - 1 - core * half


def expand_kernel(vocab, half, plan, lane_block, *refs):
    lists, (w_ref, tabr_ref, tabp_ref, cnt_ref, src, loc_s, pw_s, sem) = refs[:-8], refs[-8:]
    g = step_id()
    groups = (last_step() + 1)
    core = lax.axis_index('core')
    rows = core_rows(vocab, half)
    top = src.shape[1] // 2
    nq = top // SUB
    nblk = half // LANES
    sub = iota(SUB, LANES)
    blank = jnp.zeros((SUB, LANES), I32)

    def fetch(k):
        which = plan(k, core)
        for a, ref in enumerate(lists):
            @pl.when(which == a)
            def _():
                pltpu.make_async_copy(ref.at[:, at(lane_block(k) * LANES, LANES)], src.at[k], sem.at[k]).start()

    @pl.when(g == 0)
    def _():
        cnt_ref[...] = zeros(cnt_ref, I32)
        for k in range(src.shape[0]):
            fetch(k)

    pltpu.make_async_copy(lists[0].at[:, 0:LANES], src.at[g], sem.at[g]).wait()
    w = w_ref[...]
    over = blank
    used = blank
    first = jnp.full((SUB, LANES), nq, I32)
    prev = None
    for q in range(nq):
        order = local_order(src[g, sub8(q), :], core, half)
        ok = (order >= 0) & (order < rows)
        loc = jnp.where(ok, order, -1)
        loc_s[sub8(q), :] = loc
        pw_s[sub8(q), :] = src[g, sub8(nq + q), :] * w
        used = jnp.where(ok, q + 1, used)
        first = jnp.minimum(first, jnp.where(ok, q, nq))
        blk = loc >> 7
        if prev is not None:
            over = jnp.where((blk == prev) & ok, 1, over)
        prev = blk
    over = roll_all(over, jnp.maximum)
    lo, hi = jnp.min(first), jnp.max(used)

    def body(bt, carry):
        b0 = bt * SUB

        def scan(q, acc):
            accc, accp = list(acc[0]), list(acc[1])
            here = at(q * SUB, SUB)
            loc = loc_s[here, :]
            blk = (loc >> 7) - b0
            code = (sub + SUB * q) * LANES + (loc & (LANES - 1))
            p = pw_s[here, :]
            for i in range(SUB):
                m = blk == i
                accc[i] = jnp.where(m, code, accc[i])
                accp[i] = jnp.where(m, p, accp[i])
            return tuple(accc), tuple(accp)

        empty = (((blank - 1),) * SUB, (jnp.zeros((SUB, LANES), F32),) * SUB)
        accc, accp = lax.fori_loop(lo, hi, scan, empty)
        most = blank
        for i in range(SUB):
            code, p = accc[i], accp[i]
            head = roll_all(jnp.where(code >= 0, code, top * LANES), jnp.minimum)
            start_ = (head >> 7) & (SUB - 1)
            for sh in (1, 2, 4):
                move = (start_ & sh) != 0
                code = jnp.where(move, pltpu.roll(code, SUB - sh, 0), code)
                p = jnp.where(move, pltpu.roll(p, SUB - sh, 0), p)
            full = roll_all(jnp.where(code >= 0, sub + 1, 0), jnp.maximum)
            most = jnp.where(sub == i, full, most)
            row = at((b0 + i) * SUB, SUB)
            tabr_ref[row, :] = jnp.where(code >= 0, code & (LANES - 1), -1)
            tabp_ref[row, :] = p
        most = jnp.where(over > 0, SLOTS + 1, most)
        tile = at(b0, SUB)
        cnt_ref[tile, :] = jnp.maximum(cnt_ref[tile, :], most)
        return carry

    lax.fori_loop(0, nblk // SUB, body, 0)

    @pl.when(g == groups - 1)
    def _():
        most = jnp.max(cnt_ref[...].astype(F32), axis=1, keepdims=True)
        cnt_ref[...] = jnp.broadcast_to(most, cnt_ref.shape).astype(I32)


def expand(lists, plan, lane_block, weight, vocab, half):
    top = lists[0].shape[0] // 2
    groups = weight.shape[1] // LANES
    nblk = half // LANES
    width = groups * LANES

    def spec(rows):
        return pl.BlockSpec((rows, LANES), lambda g: (0, g))

    tabr, tabp, cnt = pl.pallas_call(
        functools.partial(expand_kernel, vocab, half, plan, lane_block),
        out_shape=(shape(nblk * SLOTS, width, I32), shape(nblk * SLOTS, width), shape(nblk, LANES, I32)),
        grid=(groups,),
        in_specs=[ANY] * len(lists) + [spec(1)],
        out_specs=(spec(nblk * SLOTS), spec(nblk * SLOTS), fixed(nblk, LANES)),
        scratch_shapes=[pltpu.VMEM((groups, 2 * top, LANES), F32), pltpu.VMEM((top, LANES), I32),
                        pltpu.VMEM((top, LANES), F32), pltpu.SemaphoreType.DMA((groups,))],
        compiler_params=params(dimension_semantics=ORDERED),
        cost_estimate=cost(groups * SMALL, 4 * width * (2 * top + 2 * nblk * SLOTS)),
    )(*lists, weight)
    return (tabr, tabp), cnt


def put_tokens(y_ref, dest, w_ref, ut_ref, u_ref):
    here = at(dest, y_ref.shape[0])
    cols = u_ref.shape[1] // 2
    ut_ref[:, here] = (y_ref[...] * (1 + w_ref[...])).astype(BF16).T
    core = lax.axis_index('core')
    for k, c in enumerate((core, 1 - core)):
        mine = at((2 * lax.axis_index('x') + c) * cols, cols)
        u_ref[here, k * cols:(k + 1) * cols] = (y_ref[:, mine] * (1 + w_ref[:, mine])).astype(BF16)


class Tokens:
    def __init__(self, srcs, buf, sem):
        self.buf = buf
        self.copies = [pltpu.make_async_copy(src, buf.at[k], sem.at[k]) for k, src in enumerate(srcs)]

    def place(self, *refs):
        core = lax.axis_index('core')
        n = self.buf.shape[1]
        for k, copy in enumerate(self.copies):
            copy.wait()
            put_tokens(self.buf.at[k], (k // 2 * 2 + (1 - core if k % 2 else core)) * n, *refs)


def tiles(vocab, half, e_ref, ut_ref, z_ref, m_ref, s_ref):
    vb = e_ref.shape[0]
    i = step_id()
    left = core_rows(vocab, half) - i * vb

    @pl.when(i == 0)
    def _():
        m_ref[...] = jnp.full(m_ref.shape, NEG, F32)
        s_ref[...] = zeros(s_ref)

    for r0 in range(0, vb, TILE):
        rs = slice(r0, r0 + TILE)
        keep = iota(TILE, WIDE) < left - r0
        for c0 in range(0, ut_ref.shape[1], WIDE):
            cs = slice(c0, c0 + WIDE)
            z = jnp.dot(e_ref[rs, :], ut_ref[:, cs], preferred_element_type=F32)
            z = jnp.where(keep, z, NEG)
            z_ref[rs, cs] = z
            z3 = z.reshape(TILE // SUB, SUB, WIDE)
            old = m_ref[:, cs]
            new = jnp.maximum(old, jnp.max(z3, axis=0))
            m_ref[:, cs] = new
            s_ref[:, cs] = s_ref[:, cs] * jnp.exp(old - new) + jnp.sum(jnp.exp(z3 - new[None]), axis=0)


def own_kernel(vocab, half, y, ypart, lists, w_ref, e_ref, z_ref, m_ref, s_ref, u_ref, lpart, ut_ref, buf, lsem, ssem, rsem):
    swap = [Links(ssem, rsem).copy(lists, lpart, other_core())]

    @pl.when(step_id() == 0)
    def _():
        tokens = Tokens((y, ypart), buf, lsem)
        start(tokens.copies)
        hello([other_core()])
        meet([other_core()])
        start(swap)
        tokens.place(w_ref, ut_ref, u_ref)

    tiles(vocab, half, e_ref, ut_ref, z_ref, m_ref, s_ref)

    @pl.when(step_id() == last_step())
    def _():
        wait(swap)


class Square:
    def __init__(self, n):
        t = lax.axis_index('tp')
        self.z, self.y, self.n = t // n, lax.rem(t, n), n
        self.zs = [lax.rem(self.z + j, n) for j in range(1, n)]
        self.ys = [lax.rem(self.y + j, n) for j in range(1, n)]
        self.along_z = [{'tp': z * n + self.y} for z in self.zs]
        self.along_y = [{'tp': self.z * n + y} for y in self.ys]
        self.peers = self.along_z + self.along_y


def x_peers(xs):
    return [along('x', 1, xs), along('x', xs - 1, xs)]


def near_kernel(xs, n, vocab, half, left, p_left, right, p_right, du, y, l_left, l_right, w_ref, e_ref,
                z_ref, m_ref, s_ref, u_ref, far0, p_far0, far1, p_far1, p_ll, p_lr, rest_ref, dw_ref,
                ut_ref, buf, a1, b1, sa, sb, a2, b2, ysl, lsem, ssem, rsem):
    i = step_id()
    sq = Square(n)
    links = Links(ssem, rsem)
    cut, part = far0.shape[0], ysl.shape[0]
    h = du.shape[3] // 2
    ahead, behind = x_peers(xs)
    core = other_core()
    tokens = Tokens((left, p_left, right, p_right), buf, lsem)
    far = [links.copy(left.at[:cut, :], far0, ahead), links.copy(right.at[cut:, :], far1, behind)]
    swap1 = [links.copy(l_left, p_ll, core), links.copy(l_right, p_lr, core)]
    swap2 = [links.copy(far0, p_far0, core), links.copy(far1, p_far1, core)]
    first, second = [], []
    for j, (z, yy, to_z, to_y) in enumerate(zip(sq.zs, sq.ys, sq.along_z, sq.along_y)):
        k = j + 1
        first.append(links.copy(du.at[:, yy, :, :h], a1.at[k], to_y))
        first.append(links.copy(du.at[z, :, :, h:], b1.at[k], to_z))
        second.append(links.copy(sa.at[z], a2.at[j], to_z))
        second.append(links.copy(sb.at[yy], b2.at[j], to_y))
    mine = [pltpu.make_async_copy(du.at[:, sq.y, :, :h], a1.at[0], lsem.at[4]),
            pltpu.make_async_copy(du.at[sq.z, :, :, h:], b1.at[0], lsem.at[5]),
            pltpu.make_async_copy(y.at[at(lax.axis_index('tp') * part, part), :], ysl, lsem.at[6])]
    peers = [core, ahead, behind, *sq.peers]

    @pl.when(i == 0)
    def _():
        start(tokens.copies)
        start(mine)
        hello(peers)
        meet(peers)
        start(first)
        start(far)
        start(swap1)
        tokens.place(w_ref, ut_ref, u_ref)

    tiles(vocab, half, e_ref, ut_ref, z_ref, m_ref, s_ref)

    @pl.when(i == last_step() - 2)
    def _():
        wait(mine)
        wait(first)
        sa[...] = total(a1)
        sb[...] = total(b1)

    @pl.when(i == last_step() - 1)
    def _():
        start(second)

    @pl.when(i == last_step())
    def _():
        wait(far)
        start(swap2)
        wait(second)
        parts = ((sa[sq.z] + total(a2), slice(h)), (sb[sq.y] + total(b2), slice(h, 2 * h)))
        dot = 0.0
        for du_sum, cs in parts:
            yv = ysl[:, cs]
            dot = dot + jnp.sum(du_sum * (1 + w_ref[:, cs]) * yv, axis=1, keepdims=True)
            dw_ref[:, cs] = jnp.sum(du_sum * yv, axis=0, keepdims=True)
        mean = dot / (2 * h)
        for du_sum, cs in parts:
            rest_ref[:, cs] = du_sum * (1 + w_ref[:, cs]) - ysl[:, cs] * mean
        wait(swap1)
        wait(swap2)


def far_kernel(xs, n, vocab, half, far0, p_far0, far1, p_far1, l_left, l_right, rest_ref, dw_ref, tz_ref, w_ref, e_ref,
               z_ref, m_ref, s_ref, u_ref, dh, l_far, p_lf, dwsum_ref, tzsum_ref,
               ut_ref, buf, xsend, xrecv, tsend, trecv, lsem, ssem, rsem):
    i = step_id()
    sq = Square(n)
    links = Links(ssem, rsem)
    h = rest_ref.shape[1] // 2
    rows = l_left.shape[0] // 2
    ahead, behind = x_peers(xs)
    tokens = Tokens((far0, p_far0, far1, p_far1), buf, lsem)
    lists = [links.copy(l_left.at[:rows, :], l_far.at[:rows, :], ahead),
             links.copy(l_right.at[rows:, :], l_far.at[rows:, :], behind)]
    swap = [links.copy(l_far, p_lf, other_core())]
    near = chip_peers(xs)
    everyone = [along('tp', j, n * n) for j in range(1, n * n)]
    xcopies = [links.copy(xsend, xrecv.at[k], to) for k, to in enumerate(near)]
    tcopies = [links.copy(tsend, trecv.at[k], to) for k, to in enumerate(everyone)]
    z, y = sq.z, sq.y
    first, second, third = [], [], []
    for to_z, to_y in zip(sq.along_z, sq.along_y):
        first.append(links.copy(rest_ref.at[:, :h], dh.at[z, y, :, :h], to_z))
        first.append(links.copy(rest_ref.at[:, h:], dh.at[z, y, :, h:], to_y))
    m = n // 2
    for to, back, low in ((0, -1, 0), (-1, 0, m)):
        yb, zb = sq.ys[back], sq.zs[back]
        second.append(links.copy(dh.at[:, y, :, :h], dh.at[:, y, :, :h], sq.along_y[to]))
        second.append(links.copy(dh.at[z, :, :, h:], dh.at[z, :, :, h:], sq.along_z[to]))
        third.append(links.copy(dh.at[low:low + m, yb, :, :h], dh.at[low:low + m, yb, :, :h], sq.along_y[to]))
        third.append(links.copy(dh.at[zb, low:low + m, :, h:], dh.at[zb, low:low + m, :, h:], sq.along_z[to]))
    mine = [pltpu.make_async_copy(rest_ref, dh.at[z, y], lsem.at[4])]
    peers = near + everyone

    @pl.when(i == 0)
    def _():
        start(tokens.copies)
        start(mine)
        hello(peers)
        xsend[...] = zeros(xsend)
        put_rows(xsend, 0, dw_ref[...])
        last = xsend.shape[0] - SUB
        xsend[last:last + 1, :] = functools.reduce(jnp.add, pieces(jnp.sum(tz_ref[...], axis=0, keepdims=True)))
        meet(peers)
        start(first)
        start(xcopies)
        start(lists)
        tokens.place(w_ref, ut_ref, u_ref)

    tiles(vocab, half, e_ref, ut_ref, z_ref, m_ref, s_ref)

    @pl.when(i == 2)
    def _():
        wait(mine)
        wait(first)
        start(second)
        wait(xcopies)
        tsend[...] = xsend[...] + total(xrecv)

    @pl.when(i == 3)
    def _():
        start(tcopies)

    @pl.when(i == last_step())
    def _():
        wait(lists)
        start(swap)
        wait(second)
        start(third)
        wait(tcopies)
        both = tsend[...] + total(trecv)
        last = both.shape[0] - SUB
        dwsum_ref[...] = to_row(both, last)
        tzsum_ref[...] = both[last:last + 1, :]
        wait(swap)
        wait(third)


def forward(kernel, ins, in_specs, scale, emb, half, vb, width, u_cols, cid, outs, scratch):
    vocab, dim = emb.shape
    nb = half // vb
    ccols = u_cols
    return pl.pallas_call(
        functools.partial(kernel, vocab, half),
        out_shape=[shape(half, width), shape(SUB, width), shape(SUB, width), shape(width, ccols, BF16)] + [o for o, _ in outs],
        grid=(nb,),
        in_specs=in_specs + [one_row(dim), pl.BlockSpec((vb, dim), lambda i: (lax.axis_index('core') * nb + i, 0))],
        out_specs=[by_row(vb, width), fixed(SUB, width), fixed(SUB, width), fixed(width, ccols)] + [o for _, o in outs],
        scratch_shapes=[pltpu.VMEM((dim, width), BF16), *scratch],
        compiler_params=comm(cid, dimension_semantics=ORDERED),
        cost_estimate=cost(2.0 * half * width * dim, half * dim * 2 + half * width * 4 + width * dim * 4, half * width),
    )(*ins, scale, emb)


def merge(m, s, ms, ss):
    best = jnp.maximum(m, jnp.max(ms, axis=0))
    return best, s * jnp.exp(m - best) + jnp.sum(ss * jnp.exp(ms - best[None]), axis=0)


def stats_kernel(tps, order, *refs):
    nlist = 2 * len(order)
    lists, refs = refs[:nlist], refs[nlist:]
    stat, refs = refs[:-12], refs[-12:]
    count_ref, c_ref, w_ref, loss_ref, pair, pairr, send, recv, out, outr, ssem, rsem = refs
    core = lax.axis_index('core')
    peers = [along('tp', j, tps) for j in range(1, tps)]
    partner = other_core()
    everyone = [partner, *peers]
    hello(everyone)
    gr = pair.shape[0] // 2
    base = 0
    pair[...] = zeros(pair)
    for m_ref, s_ref in zip(stat[::2], stat[1::2]):
        m = jnp.max(m_ref[...], axis=0, keepdims=True)
        s = jnp.sum(s_ref[...] * jnp.exp(m_ref[...] - m), axis=0, keepdims=True)
        put_rows(pair, base, m)
        put_rows(pair, gr + base, s)
        base += m.shape[1] // LANES
    masks = []
    for chip, cuts in enumerate(order):
        for lanes in cuts:
            a, b = (ref[0:1, lanes] for ref in lists[2 * chip:2 * chip + 2])
            masks += [jnp.where(core == 0, a, b), jnp.where(core == 0, b, a)]
    mask = (jnp.concatenate(masks, axis=1) > 0).astype(F32)
    w = mask / count_ref[:, 0:1]
    w_ref[...] = w

    links = Links(ssem, rsem)
    both = [links.copy(pair, pairr, partner)]
    copies = [links.copy(send, recv.at[k], to) for k, to in enumerate(peers)]
    back = [links.copy(out, outr, partner)]
    meet(everyone)
    start(both)
    wait(both)
    m, s = merge(pair[:gr, :], pair[gr:, :], pairr[:gr, :][None], pairr[gr:, :][None])
    hg = base // 2
    mine, mid = slice(hg), slice(SUB, SUB + hg)
    send[...] = zeros(send)
    for rows, x in ((mine, m), (mid, s)):
        send[rows, :] = jnp.where(core == 0, x[:hg, :], x[hg:base, :])
    start(copies)
    wait(copies)
    m, s = merge(send[mine, :], send[mid, :], recv[:, mine, :], recv[:, mid, :])
    out[...] = zeros(out)
    out[mine, :] = m + jnp.log(s)
    start(back)
    wait(back)
    a, b = out[mine, :], outr[mine, :]
    lse = jnp.concatenate([jnp.where(core == 0, a, b), jnp.where(core == 0, b, a)], axis=0)
    lse = to_row(lse, base)
    c_ref[...] = jnp.where(mask > 0, lse - jnp.log(w), BIG)
    loss_ref[...] = functools.reduce(jnp.add, pieces(w * lse))


def stats(lists, order, stat, count, tps, cid):
    width = sum(m.shape[1] for m in stat[::2])
    gr = -(-width // (LANES * SUB)) * SUB
    pair, some, line_ = (pltpu.VMEM((rows, LANES), F32) for rows in (2 * gr, 2 * SUB, SUB))
    return pl.pallas_call(
        functools.partial(stats_kernel, tps, order),
        out_shape=[line(width), line(width), line(LANES)],
        grid=(1,),
        in_specs=[fixed(SUB, lists[0].shape[1])] * len(lists) + [fixed(*a.shape) for a in (*stat, count)],
        out_specs=[one_row(width), one_row(width), one_row(LANES)],
        scratch_shapes=[pair, pair, some, pltpu.VMEM((tps - 1, 2 * SUB, LANES), F32), line_, line_, *dmas(tps + 1)],
        compiler_params=comm(cid),
        cost_estimate=cost(SMALL, 1 << 16),
    )(*lists, *stat, count)


def fill_teacher(cnt_ref, first, nrb, tabr_ref, tabp_ref, w_ref, lists, plan, lane_block, half, tm, src, sem):
    width = tm.shape[1]
    core = lax.axis_index('core')
    rows = iota(LANES, LANES)
    zero = jnp.zeros((LANES, LANES), F32)
    top = src.shape[0] // 2

    def pick(row, val, t):
        for s in range(SUB):
            t = jnp.where(rows == row[s:s + 1, :], val[s:s + 1, :], t)
        return t

    for rb in range(nrb):
        n = cnt_ref[first + rb, 0]
        rs = slice(rb * LANES, (rb + 1) * LANES)

        def tile(g, carry):
            lanes = at(g * LANES, LANES)

            @pl.when(n <= SLOTS)
            def _():
                tm[rs, lanes] = pick(tabr_ref[sub8(rb), lanes], tabp_ref[sub8(rb), lanes], zero)

            @pl.when(n > SLOTS)
            def _():
                which = plan(g, core)
                for a, ref in enumerate(lists):
                    @pl.when(which == a)
                    def _():
                        copy = pltpu.make_async_copy(ref.at[:, at(lane_block(g) * LANES, LANES)], src, sem.at[0])
                        copy.start()
                        copy.wait()
                w = w_ref[:, lanes]

                def entries(k, t):
                    order = local_order(src[at(k * SUB, SUB), :], core, half) - (first + rb) * LANES
                    return pick(order, src[at(top + k * SUB, SUB), :] * w, t)

                tm[rs, lanes] = lax.fori_loop(0, top // SUB, entries, zero)

            return carry

        lax.fori_loop(0, width // LANES, tile, 0)


class Ring:
    def __init__(self, srcs, b0, buf, sem):
        self.srcs, self.b0, self.buf, self.sem = srcs, b0, buf, sem

    def copies(self, k):
        depth, rows = self.buf.shape[:2]
        slot = lax.rem(k, depth)
        c0 = 0
        for a, src in enumerate(self.srcs):
            c1 = c0 + src.shape[1]
            yield pltpu.make_async_copy(src.at[at((self.b0 + k) * rows, rows), :], self.buf.at[slot, :, c0:c1],
                                        self.sem.at[slot, a])
            c0 = c1

    def turn(self, i, last):
        ahead = self.buf.shape[0] - 1

        @pl.when(i == 0)
        def _():
            for k in range(ahead):
                start(self.copies(k))

        @pl.when(i + ahead <= last)
        def _():
            start(self.copies(i + ahead))

        wait(self.copies(i))
        return self.buf.at[lax.rem(i, ahead + 1)]


def ring_scratch(rows, cols, n):
    return [pltpu.VMEM((3, rows, cols), F32), pltpu.SemaphoreType.DMA((3, n))]


def g_tile(z_ref, z0, c_ref, cs, rb, tabr_ref, tabp_ref, tm, put):
    c = c_ref[:, cs]
    step = 2 * SUB
    rows = iota(step, TILE)
    slots = range(SUB * rb, SUB * rb + FAST)
    ids = [jnp.broadcast_to(tabr_ref[s:s + 1, cs], (step, TILE)) for s in slots]
    vals = [tabp_ref[s:s + 1, cs] for s in slots]
    for r0 in range(0, LANES, step):
        rs = slice(rb * LANES + r0, rb * LANES + r0 + step)
        z = z_ref[rs, z0:z0 + TILE]
        if tm is None:
            t = jnp.zeros((step, TILE), F32)
            for row, val in zip(ids, vals):
                t = jnp.where(rows + r0 == row, val, t)
        else:
            t = tm[rs, cs]
        put(rs, (jnp.exp(z - c) - t).astype(BF16), t, z)


def most_slots(cnt_ref, first, nrb):
    n = cnt_ref[first, 0]
    for rb in range(1, nrb):
        n = jnp.maximum(n, cnt_ref[first + rb, 0])
    return n


def fill_scratch(vb, width, lists):
    return [pltpu.VMEM((vb, width), F32), pltpu.VMEM((lists[0].shape[0], LANES), F32), pltpu.SemaphoreType.DMA((1,))]


def g_kernel(half, plan, lane_block, cnt_ref, z_hbm, c_ref, tabr_ref, tabp_ref, w_ref, *refs):
    lists, (g_ref, gt_ref, tz_ref, tm, src, sem, zbuf, zsem) = refs[:-8], refs[-8:]
    i = step_id()
    vb, width = g_ref.shape
    z_ref = Ring((z_hbm,), 0, zbuf, zsem).turn(i, last_step())
    nrb = vb // LANES

    @pl.when(i == 0)
    def _():
        tz_ref[...] = zeros(tz_ref)

    slots = most_slots(cnt_ref, i * nrb, nrb)

    def make(full):
        for c0 in range(0, width, TILE):
            cs = slice(c0, c0 + TILE)
            acc = [jnp.zeros((SUB, TILE), F32)]

            def put(rs, g, t, z):
                g_ref[rs, cs] = g
                tz = t * z
                acc[0] = acc[0] + tz[:SUB] + tz[SUB:]

            for rb in range(nrb):
                g_tile(z_ref, c0, c_ref, cs, rb, tabr_ref, tabp_ref, full, put)
                rs = slice(rb * LANES, (rb + 1) * LANES)
                gt_ref[cs, rs] = g_ref[rs, cs].T
            tz_ref[:, cs] += acc[0]

    @pl.when(slots <= FAST)
    def _():
        make(None)

    @pl.when(slots > FAST)
    def _():
        fill_teacher(cnt_ref, i * nrb, nrb, tabr_ref, tabp_ref, w_ref, lists, plan, lane_block, half, tm, src, sem)
        make(tm)


def g_own(cnt, z, c, tables, w, lists, plan, lane_block):
    half, width = z.shape
    vb = 2 * WIDE
    trows = vb // LANES * SLOTS

    def row(i, n):
        return (i, 0)

    return pl.pallas_call(
        functools.partial(g_kernel, half, plan, lane_block),
        out_shape=(shape(half, width, BF16), shape(width, half, BF16), shape(SUB, width)),
        grid_spec=pltpu.PrefetchScalarGridSpec(
            num_scalar_prefetch=1,
            grid=(half // vb,),
            in_specs=[ANY, one_row(width), pl.BlockSpec((trows, width), row),
                      pl.BlockSpec((trows, width), row), one_row(width)] + [ANY] * len(lists),
            out_specs=(pl.BlockSpec((vb, width), row), pl.BlockSpec((width, vb), lambda i, n: (0, i)), fixed(SUB, width)),
            scratch_shapes=fill_scratch(vb, width, lists) + ring_scratch(vb, width, 1),
        ),
        compiler_params=params(dimension_semantics=ORDERED),
        cost_estimate=cost(LARGE, half * width * 8, half * width),
        name='g_own',
    )(cnt, z, c, *tables, w, *lists)


def du_kernel(vocab, half, gt_ref, left, right, e_ref, out_ref, p_left, p_right, mine, send, recv, ssem, rsem):
    i = step_id()
    core = lax.axis_index('core')
    rows = core_rows(vocab, half)
    tok = out_ref.shape[0]
    tiles = last_step() - 1
    cut = (vocab - half) // TILE * TILE
    links = Links(ssem, rsem)
    swap = [links.copy(left, p_left, other_core()), links.copy(right, p_right, other_core())]

    @pl.when(i == 0)
    def _():
        hello([other_core()])
        meet([other_core()])
        start(swap)

    def copy(k):
        return pltpu.make_async_remote_copy(
            src_ref=send.at[k], dst_ref=recv.at[k], send_sem=ssem.at[2 + k], recv_sem=rsem.at[2 + k],
            device_id=other_core(), device_id_type=MESH)

    @pl.when((i >= 1) & (i <= tiles))
    def _():
        copy(i - 1).start()

    @pl.when(i < tiles)
    def _():
        tail = e_ref[cut:, :]
        tail = jnp.where(iota(*tail.shape) < rows - cut, tail, jnp.zeros((), BF16))

        def part(which):
            g = gt_ref[at(which * tok, tok), :]
            return (jnp.dot(g[:, :cut], e_ref[:cut, :], preferred_element_type=F32)
                    + jnp.dot(g[:, cut:], tail, preferred_element_type=F32))

        send[i] = part(1 - core)
        mine[i] = part(core)

    @pl.when(i >= 2)
    def _():
        copy(i - 2).wait()
        out_ref[...] = mine[i - 2] + recv[i - 2]

    @pl.when(i == last_step())
    def _():
        wait(swap)


def du_call(gt, left, right, emb, half):
    vocab, dim = emb.shape
    tok = gt.shape[0] // 2
    n = dim // WIDE
    buf = pltpu.VMEM((n, tok, WIDE), F32)
    near = shape(*left.shape)
    return pl.pallas_call(
        functools.partial(du_kernel, vocab, half),
        out_shape=(shape(tok, dim), near, near),
        grid=(n + 2,),
        in_specs=[fixed(*gt.shape), ANY, ANY,
                  pl.BlockSpec((half, WIDE), lambda i: (lax.axis_index('core'), jnp.minimum(i, n - 1)))],
        out_specs=(pl.BlockSpec((tok, WIDE), lambda i: (0, jnp.maximum(i - 2, 0))), ANY, ANY),
        scratch_shapes=[buf, buf, buf, *dmas(n + 2)],
        compiler_params=comm(2, dimension_semantics=ORDERED),
        cost_estimate=cost(4.0 * half * tok * dim, half * dim * 2),
        name='grad_u',
    )(gt, left, right, emb)


def de_kernel(half, b0, nu, plan, lane_block, cnt_ref, *refs):
    u_refs, refs = refs[:nu], refs[nu:]
    zn, zf, gown_ref, c_ref, tabr_ref, tabp_ref, w_ref = refs[:7]
    lists = refs[7:13]
    out_ref, part_ref, u_ref, g_ref, tm, src, sem, zbuf, zsem = refs[-9:]
    i = step_id()
    vb, mine = gown_ref.shape
    cols = out_ref.shape[1]
    nrb = vb // LANES
    first = (b0 + i) * nrb
    z_ref = Ring((zn, zf), b0, zbuf, zsem).turn(i, last_step())

    @pl.when(i == 0)
    def _():
        base = 0
        for ref in u_refs:
            u_ref[base:base + ref.shape[0], :] = ref[...]
            base += ref.shape[0]

    def make(full):
        for r0 in range(0, vb, TILE):
            rows = slice(r0, r0 + TILE)
            acc = jnp.dot(gown_ref[rows, :], u_ref[:mine, :], preferred_element_type=F32)
            for c0 in range(0, g_ref.shape[1], TILE):
                cs = slice(c0, c0 + TILE)

                def put(rs, g, t, z):
                    g_ref[rs, cs] = g

                for rb in range(r0 // LANES, (r0 + TILE) // LANES):
                    g_tile(z_ref, c0, c_ref, cs, rb, tabr_ref, tabp_ref, full, put)
                acc = acc + jnp.dot(g_ref[rows, cs], u_ref[mine + c0:mine + c0 + TILE, :], preferred_element_type=F32)
            out_ref[rows, :] = acc[:, :cols]
            part_ref[rows, :] = acc[:, cols:]

    slots = most_slots(cnt_ref, first, nrb)

    @pl.when(slots <= FAST)
    def _():
        make(None)

    @pl.when(slots > FAST)
    def _():
        fill_teacher(cnt_ref, first, nrb, tabr_ref, tabp_ref, w_ref, lists, plan, lane_block, half, tm, src, sem)
        make(tm)


def de_call(cnt, us, zn, zf, gown, c, tables, w, lists, plan, lane_block, vocab, b0, nb, prev):
    half, mine = gown.shape
    ccols = us[0].shape[1]
    cols = ccols // 2
    vb = WIDE
    tot = half // vb
    width = zn.shape[1] + zf.shape[1]
    trows = vb // LANES * SLOTS

    def rows(cols_, height=vb):
        return pl.BlockSpec((height, cols_), lambda i, n: (b0 + i, 0))

    in_specs = [fixed(*u.shape) for u in us]
    in_specs += [ANY, ANY, rows(mine), one_row(width), rows(width, trows), rows(width, trows), one_row(width)]
    in_specs += [ANY] * len(lists)
    args = [*us, zn, zf, gown, c, *tables, w, *lists]
    aliases = {}
    if prev is not None:
        aliases = {1 + len(args): 0}
        args.append(prev)
        in_specs.append(ANY)
    return pl.pallas_call(
        functools.partial(de_kernel, half, b0, len(us), plan, lane_block),
        out_shape=(shape(vocab, cols), shape(nb * vb, cols)),
        grid_spec=pltpu.PrefetchScalarGridSpec(
            num_scalar_prefetch=1,
            grid=(nb,),
            in_specs=in_specs,
            out_specs=(
                pl.BlockSpec((vb, cols), lambda i, n: (lax.axis_index('core') * tot + b0 + i, 0)),
                pl.BlockSpec((vb, cols), lambda i, n: (i, 0)),
            ),
            scratch_shapes=[pltpu.VMEM((width + mine, ccols), BF16), pltpu.VMEM((vb, width), BF16),
                            *fill_scratch(vb, width, lists), *ring_scratch(vb, width, 2)],
        ),
        input_output_aliases=aliases,
        compiler_params=params(dimension_semantics=ORDERED),
        cost_estimate=cost(3.0 * nb * vb * (width + mine) * ccols, nb * vb * (width * 4 + mine * 2 + ccols * 4),
                           nb * vb * width),
    )(cnt, *args)


def place_kernel(half_blocks, a_ref, b_ref, prev_ref, out_ref):
    i = step_id()
    for k, ref in enumerate((a_ref, b_ref)):
        @pl.when(i // half_blocks == k)
        def _():
            out_ref[...] = ref[...]


def place(recvs, out, half):
    cols = out.shape[1]
    step = 2 * WIDE
    n = recvs[0].shape[0] // step
    return pl.pallas_call(
        functools.partial(place_kernel, n),
        out_shape=shape(*out.shape),
        grid=(2 * n,),
        in_specs=[pl.BlockSpec((step, cols), lambda i: (jnp.minimum(i, n - 1), 0)),
                  pl.BlockSpec((step, cols), lambda i: (jnp.maximum(i - n, 0), 0)), ANY],
        out_specs=pl.BlockSpec((step, cols), lambda i: ((1 - lax.axis_index('core')) * (half // step) + i, 0)),
        input_output_aliases={2: 0},
        compiler_params=params(),
        cost_estimate=cost(SMALL, out.size * 4),
        name='place',
    )(*recvs, out)


def dh_kernel(d_ref, inv_ref, out_ref):
    out_ref[...] = (inv_ref[...] * d_ref[...]).astype(BF16)


def dh_call(d, inv):
    tok, dim = d.shape
    step = tok // 4
    return pl.pallas_call(
        dh_kernel,
        out_shape=shape(tok, dim, BF16),
        grid=(tok // step,),
        in_specs=[by_row(step, dim), by_row(step, 1)],
        out_specs=by_row(step, dim),
        compiler_params=params(),
        cost_estimate=cost(SMALL, tok * dim * 6),
        name='grad_h',
    )(d, inv)


def solution(mesh):
    tps = mesh.shape['tp']
    xs = mesh.shape['dp'] // 2
    n = round(tps ** 0.5)
    grid = Mesh(np.asarray(mesh.devices).reshape(tps, xs, 2), ('tp', 'x', 'core'))

    def shift(x, axis, by):
        size = grid.shape[axis]
        return lax.ppermute(x, axis, [(i, (i + by) % size) for i in range(size)])

    def local_head(hidden, embedding, norm_weight, teach_ids, teach_prob, tok_mask):
        vocab, dim = embedding.shape
        tok = hidden.shape[0]
        chip = 2 * tok
        half = -(-vocab // (2 * WIDE)) * WIDE
        part = tok // tps
        cut = tok // 2
        tg = tok // LANES
        weight = norm_weight.reshape(row_of(norm_weight))
        mask = tok_mask.reshape(row_of(tok_mask))
        ccols = dim // xs
        dma = pltpu.SemaphoreType.DMA

        normed, inv_rms, count = norm(hidden, mask, xs)
        left = shift(normed, 'x', 1)
        right = shift(normed, 'x', -1)
        lists, y_part = sort_lists(teach_ids, teach_prob, mask, normed, vocab, vocab * tps)
        l_left = shift(lists, 'x', 1)
        l_right = shift(lists, 'x', -1)
        some_lists = (shape(*lists.shape), ANY)

        z0, m0, s0, u0, l_part = forward(
            own_kernel, [normed, y_part, lists], [ANY] * 3, weight, embedding, half, 2 * WIDE, chip, ccols, 5,
            [some_lists], [pltpu.VMEM((2, tok, dim), F32), dma((2,)), *dmas(1)])
        full = slice(tok)
        lo, hi = slice(cut), slice(cut, tok)
        c0, w0, loss0 = stats([lists, l_part], ((full,),), (m0, s0), count, tps, 0)
        own_plan = (lambda g, c: lax.rem(g // tg + c, 2)), (lambda g: lax.rem(g, tg))
        tab0, cnt0 = expand([lists, l_part], *own_plan, w0, vocab, half)
        g0, gt0, tz = g_own(cnt0, z0, c0, tab0, w0, [lists, l_part], *own_plan)
        du, p_left, p_right = du_call(gt0, left, right, embedding, half)

        square = pltpu.VMEM((n, n, part, dim // 2), F32)
        strip = pltpu.VMEM((n, part, dim // 2), F32)
        short = pltpu.VMEM((n - 1, part, dim // 2), F32)
        some_far = (shape(cut, dim), ANY)
        z1, m1, s1, u1, far0, p_far0, far1, p_far1, p_ll, p_lr, d_rest, dw = forward(
            functools.partial(near_kernel, xs, n),
            [left, p_left, right, p_right, du.reshape(n, n, part, dim), normed, l_left, l_right], [ANY] * 8,
            weight, embedding, half, WIDE, 2 * chip, ccols, 3,
            [some_far] * 4 + [some_lists] * 2 + [(shape(part, dim), fixed(part, dim)), (line(dim), one_row(dim))],
            [pltpu.VMEM((4, tok, dim), F32), square, square, strip, strip, short, short, pltpu.VMEM((part, dim), F32),
             dma((7,)), *dmas(6 + 4 * (n - 1))])
        sums = pltpu.VMEM((dim // LANES + SUB, LANES), F32)

        def many(k):
            return pltpu.VMEM((k - 1, dim // LANES + SUB, LANES), F32)

        z2, m2, s2, u2, dh, l_far, p_lf, dw_sum, tz_sum = forward(
            functools.partial(far_kernel, xs, n), [far0, p_far0, far1, p_far1, l_left, l_right, d_rest, dw, tz],
            [ANY] * 6 + [fixed(part, dim), one_row(dim), fixed(*tz.shape)],
            weight, embedding, half, WIDE, chip, ccols, 6,
            [(jax.ShapeDtypeStruct((n, n, part, dim), F32), ANY), some_lists, some_lists,
             (line(dim), one_row(dim)), (line(LANES), one_row(LANES))],
            [pltpu.VMEM((4, cut, dim), F32), sums, many(2 * xs), sums, many(tps), dma((5,)),
             *dmas(3 + 2 * xs - 1 + tps - 1 + 2 * (n - 1) + 8)])
        l_rest = [l_left, p_ll, l_right, p_lr, l_far, p_lf]
        c1, w1, loss1 = stats(l_rest, ((full,), (full,), (lo, hi)), (m1, s1, m2, s2), count, tps, 1)

        def plan(g, c):
            far = g // (2 * tg) == 2
            swap = jnp.where(far, lax.rem(g, 2), lax.rem(g // tg, 2))
            return g // (2 * tg) * 2 + lax.rem(swap + c, 2)

        def lane_block(g):
            return jnp.where(g // (2 * tg) == 2, lax.rem(g // 2, tg), lax.rem(g, tg))

        rest_plan = plan, lane_block
        tab1, cnt1 = expand(l_rest, *rest_plan, w1, vocab, half)

        nb = half // WIDE
        n0 = nb // 2

        def grad_e(b0, count_, prev):
            return de_call(cnt1, [u0, u1, u2], z1, z2, g0, c1, tab1, w1, l_rest, *rest_plan, vocab, b0, count_, prev)

        out, send0 = grad_e(0, n0, None)
        recv0 = shift(send0, 'core', 1)
        out, send1 = grad_e(n0, nb - n0, out)
        recv1 = shift(send1, 'core', 1)
        grad_hidden = dh_call(dh.reshape(tok, dim), inv_rms)
        out = place([recv0, recv1], out, half)
        return jnp.sum(loss0 + loss1 - tz_sum), grad_hidden, out, dw_sum.reshape(dim)

    tokens = ('x', 'core')
    return jax.shard_map(
        local_head,
        mesh=grid,
        in_specs=(P(tokens, None), P('tp', None), P(None), P(tokens, None), P(tokens, None), P(tokens)),
        out_specs=(P(), P(tokens, None), P('tp', tokens), P(None)),
        check_vma=False,
    )
```
